256 devices in a mesh: batch: 16 (over x_lo, z), seq: 16 (over x_hi, y, core).
Axes of the slice: x: 4 (x_hi: 2, x_lo: 2; x = x_hi * 2 + x_lo), y: 4, z: 8, core: 2. Of those that a mesh axis runs over, the one named last changes fastest.
Arguments:
- hidden_in: bfloat16 [16, 2048, 2048], P('batch', 'seq'), may hold values from -6 to 6
- queries: bfloat16 [16, 2048, 2048], P('batch', 'seq'), may hold values from -5 to 5
- key_states: bfloat16 [16, 2048, 512], P('batch', 'seq'), may hold values from -12 to 12
- value_states: bfloat16 [16, 2048, 512], P('batch', 'seq'), may hold values from -6 to 6
- grad_out: bfloat16 [16, 2048, 2048], P('batch', 'seq'), may hold values from -6 to 6
- log_sums: float32 [16, 16, 2048], P('batch', None, 'seq'), may hold values from -700 to 700, as said below
- deltas: float32 [16, 16, 2048], P('batch', None, 'seq'), may hold values from -6 to 6
- block_order: int32 [32], replicated, may hold values from 0 to 31, as said below
Outputs:
- grad_queries: bfloat16 [16, 2048, 2048], P('batch', 'seq')
- grad_keys: bfloat16 [16, 2048, 512], P('batch', 'seq')
- grad_values: bfloat16 [16, 2048, 512], P('batch', 'seq')
- key_wgrad: float32 [2048, 512], P(('batch', 'seq'))
- value_wgrad: float32 [2048, 512], P(('batch', 'seq'))
The draws below stay inside these ranges and needn't reach their ends.
Inputs may be any that keep to these rules, and one draw needn't show every extreme that they name: `block_order`: entries 2i and 2i+1 name blocks c and 31 - c for some c, in either order; the 32 entries together are a permutation of 0 to 31. `log_sums`: each entry lies within 0.1 of the log of the sum over visible j of exp(scores[b,h,i,j]).
All inputs are finite; a program needn't handle non-finite values.
Results may differ from the reference program's by a relative error of at most 0.0049.
Values may be sent and summed in bfloat16 or wider, within the bound.
A program may use at most 64 MiB of HBM per device.

```python
import math
import jax
import jax.numpy as jnp
from jax import lax

HQ = 16
HK = 4
DH = 128
DIN = 2048
SEQ = 2048
BATCH = 16
BLOCK = 64
BLOCKS = 32
GROUP = 4
QW = 2048
KW = 512


def draw_queries(key, part):
    normal_part = jnp.clip(jax.random.normal(jax.random.fold_in(key, 11), (BATCH, SEQ, HQ * DH), jnp.float32), -4.0, 4.0)
    return normal_part.astype(jnp.bfloat16)


def draw_key_states(key, part):
    normal_part = jnp.clip(jax.random.normal(jax.random.fold_in(key, 13), (BATCH, SEQ, HK * DH), jnp.float32), -4.0, 4.0)
    return normal_part.astype(jnp.bfloat16)


def draw_block_order(key, part):
    pair_key, flip_key = jax.random.split(jax.random.fold_in(key, 29))
    pair_ids = jax.random.permutation(pair_key, BLOCKS // 2).astype(jnp.int32)
    flip_bits = jax.random.randint(flip_key, (BLOCKS // 2,), 0, 2)
    first_block = jnp.where(flip_bits == 1, BLOCKS - 1 - pair_ids, pair_ids)
    second_block = BLOCKS - 1 - first_block
    return jnp.stack([first_block, second_block], axis=1).reshape(BLOCKS).astype(jnp.int32)


def draw_log_sums(key, part):
    query_all = draw_queries(key, part).astype(jnp.float32)
    key_all = draw_key_states(key, part).astype(jnp.float32)
    order = draw_block_order(key, part)
    row_ids = jnp.arange(SEQ, dtype=jnp.int32)
    position = order[row_ids // BLOCK] * BLOCK + row_ids % BLOCK
    visible = position[None, :] <= position[:, None]

    def one_group(group_ops):
        group_queries, group_keys = group_ops
        scores = jnp.einsum('igd,jd->gij', group_queries, group_keys) * (1.0 / math.sqrt(DH))
        scores = jnp.where(visible[None, :, :], scores, -jnp.inf)
        return jax.nn.logsumexp(scores, axis=-1)

    def one_sequence(seq_ops):
        seq_queries, seq_keys = seq_ops
        queries_head = jnp.moveaxis(seq_queries.reshape(SEQ, HK, GROUP, DH), 1, 0)
        keys_head = jnp.moveaxis(seq_keys.reshape(SEQ, HK, DH), 1, 0)
        return lax.map(one_group, (queries_head, keys_head)).reshape(HQ, SEQ)
    exact = lax.map(one_sequence, (query_all, key_all))
    noise = jax.random.uniform(jax.random.fold_in(key, 41), (BATCH, HQ, SEQ), jnp.float32, -0.1, 0.1)
    return (exact + noise).astype(jnp.float32)


def spiked(result, stream_key, source, target, blocks, factor):
    def block_of(dim):
        return (jnp.arange(result.shape[dim]) // (result.shape[dim] // blocks)).reshape((-1,) + (1,) * (result.ndim - 1 - dim))

    one_side = jax.random.permutation(stream_key, blocks)[block_of(target)]
    far = (block_of(target) + blocks // 2) % blocks
    return jnp.where((block_of(source) == one_side) | (block_of(source) == far), factor * result, result)


def block_scale(rng, shape, cuts, smallest, top_value):
    def one(dim, blocks):
        steps = jax.random.uniform(jax.random.fold_in(jax.random.fold_in(rng, 6), dim), (blocks,), jnp.float32, smallest / len(cuts), top_value / len(cuts))
        return jnp.repeat(jnp.exp(steps), shape[dim] // blocks).reshape((-1,) + (1,) * (len(shape) - dim - 1))

    factor_of = one(*cuts[0])
    for cut in cuts[1:]:
        factor_of = factor_of * one(*cut)
    return factor_of


def scatter_about(rng, dims, width, reach, cuts=(), kind=jnp.bfloat16):
    loudness = block_scale(rng, dims, cuts, -0.22, 0.18) if cuts else 1.0
    entries = jax.random.normal(rng, dims, jnp.float32) * width * loudness
    return jnp.minimum(jnp.maximum(entries, -reach), reach).astype(kind)


def heavy_noise(rng, dims, width, reach, cuts, heavy, held_as=jnp.bfloat16):
    result = width * jax.random.normal(rng, dims, jnp.float32)
    if cuts:
        result = result * block_scale(rng, dims, cuts, -0.22, 0.18)
    return jnp.clip(spiked(result, jax.random.fold_in(rng, 3), *heavy), -reach, reach).astype(held_as)


def setup_inputs(seed: int = 0) -> dict:
    arg_keys = jax.random.split(jax.random.key(seed), 9)
    hidden_in = heavy_noise(arg_keys[0], (BATCH, SEQ, DIN), 1.0, 6.0, ((0, 16), (1, 16)), (1, 2, 16, 2.0))
    queries = draw_queries(jax.random.fold_in(arg_keys[8], 71), 0)
    key_states = draw_key_states(jax.random.fold_in(arg_keys[8], 71), 0)
    value_states = scatter_about(arg_keys[3], (BATCH, SEQ, KW), 1.0, 6.0, ((0, 16), (1, 16)))
    grad_out = scatter_about(arg_keys[4], (BATCH, SEQ, QW), 1.0, 6.0, ((0, 16), (1, 16)))
    log_sums = draw_log_sums(jax.random.fold_in(arg_keys[8], 71), 0)
    deltas = scatter_about(arg_keys[6], (BATCH, HQ, SEQ), 1.0, 6.0, ((0, 16), (2, 16)), jnp.float32)
    block_order = draw_block_order(jax.random.fold_in(arg_keys[8], 71), 0)
    return {"hidden_in": hidden_in, "queries": queries, "key_states": key_states, "value_states": value_states, "grad_out": grad_out, "log_sums": log_sums, "deltas": deltas, "block_order": block_order}


def group_grads(operands, position):
    group_queries, group_keys, group_values, group_cots, group_lse, group_deltas = operands
    scale_factor = 1.0 / math.sqrt(DH)
    query_full = group_queries.astype(jnp.float32)
    key_full = group_keys.astype(jnp.float32)
    value_full = group_values.astype(jnp.float32)
    grad_full = group_cots.astype(jnp.float32)
    scores = jnp.einsum('igd,jd->gij', query_full, key_full) * scale_factor
    visible = position[None, :] <= position[:, None]
    scores = jnp.where(visible[None, :, :], scores, -jnp.inf)
    probs = jnp.exp(scores - group_lse[..., None])
    grad_probs = jnp.einsum('igd,jd->gij', grad_full, value_full)
    grad_scores = (probs * (grad_probs - group_deltas[..., None]) * scale_factor).astype(jnp.bfloat16)
    grad_scores = lax.optimization_barrier(grad_scores).astype(jnp.float32)
    probs_low = lax.optimization_barrier(probs.astype(jnp.bfloat16)).astype(jnp.float32)
    query_grad = jnp.einsum('gij,jd->igd', grad_scores, key_full)
    key_grad = jnp.einsum('gij,igd->jd', grad_scores, query_full)
    value_grad = jnp.einsum('gij,igd->jd', probs_low, grad_full)
    return (query_grad, key_grad, value_grad)

def sequence_grads(operands, position):
    seq_queries, seq_keys, seq_values, seq_cots, seq_lse, seq_deltas = operands
    group_size = HQ // HK
    queries_head = jnp.moveaxis(seq_queries.reshape(SEQ, HK, group_size, DH), 1, 0)
    keys_head = jnp.moveaxis(seq_keys.reshape(SEQ, HK, DH), 1, 0)
    values_head = jnp.moveaxis(seq_values.reshape(SEQ, HK, DH), 1, 0)
    cots_head = jnp.moveaxis(seq_cots.reshape(SEQ, HK, group_size, DH), 1, 0)
    lse_head = seq_lse.reshape(HK, group_size, SEQ)
    deltas_head = seq_deltas.reshape(HK, group_size, SEQ)
    query_grad, key_grad, value_grad = lax.map(lambda group_ops: group_grads(group_ops, position), (queries_head, keys_head, values_head, cots_head, lse_head, deltas_head))
    query_grad = jnp.moveaxis(query_grad, 0, 1).reshape(SEQ, HQ * DH)
    key_grad = jnp.moveaxis(key_grad, 0, 1).reshape(SEQ, HK * DH)
    value_grad = jnp.moveaxis(value_grad, 0, 1).reshape(SEQ, HK * DH)
    return (query_grad.astype(jnp.bfloat16), key_grad.astype(jnp.bfloat16), value_grad.astype(jnp.bfloat16))

def reference(hidden_in, queries, key_states, value_states, grad_out, log_sums, deltas, block_order):
    row_ids = jnp.arange(SEQ, dtype=jnp.int32)
    position = (block_order[row_ids // BLOCK] * BLOCK + row_ids % BLOCK).astype(jnp.int32)
    grad_queries, grad_keys, grad_values = lax.map(lambda seq_ops: sequence_grads(seq_ops, position), (queries, key_states, value_states, grad_out, log_sums, deltas))
    flat_hidden = hidden_in.reshape(BATCH * SEQ, DIN)
    key_wgrad = jnp.dot(flat_hidden.T, grad_keys.reshape(BATCH * SEQ, HK * DH), preferred_element_type=jnp.float32)
    value_wgrad = jnp.dot(flat_hidden.T, grad_values.reshape(BATCH * SEQ, HK * DH), preferred_element_type=jnp.float32)
    return (grad_queries, grad_keys, grad_values, key_wgrad, value_wgrad)
```

```python
import functools
import math

import jax
import jax.numpy as jnp
from jax import lax
from jax.experimental import pallas as pl
from jax.experimental.pallas import tpu as pltpu
from jax.sharding import PartitionSpec as P

MESH = pl.DeviceIdType.MESH
HQ = 16
HK = 4
DH = 128
SCALE = 1.0 / math.sqrt(DH)
LOG2E = math.log2(math.e)
BF = jnp.bfloat16
F32 = jnp.float32


def place():
    b, s = lax.axis_index("batch"), lax.axis_index("seq")
    return b, s, s // 8, (s // 2) % 4, s % 2


def seq_of(xh, y, c):
    return xh * 8 + y * 2 + c


def near(b, xh, y, c):
    along = [(b, seq_of(xh, (y + d) % 4, c)) for d in (1, 2, 3)]
    return along, (b, seq_of(xh, y, 1 - c)), (b, seq_of(1 - xh, y, c))


def remote(src, dst, send, recv, dev):
    copy = pltpu.make_async_remote_copy(
        src_ref=src,
        dst_ref=dst,
        send_sem=send,
        recv_sem=recv,
        device_id=dev,
        device_id_type=MESH,
    )
    copy.start()
    return copy


def signal(sem, dev):
    pl.semaphore_signal(sem, inc=1, device_id=dev, device_id_type=MESH)


def lanes(index, width):
    return pl.ds(pl.multiple_of(index * width, width), width)


def gather_kernel(q, do, k, v, ld, qx, dox, kvx, ldx, ssem, rsem, lsem):
    b, s, xh, y, c = place()
    along, partner, across = near(b, xh, y, c)
    barrier = pltpu.get_barrier_semaphore()
    for dev in (*along, partner, across):
        signal(barrier, dev)
    pl.semaphore_wait(barrier, 5)

    own_k = pltpu.make_async_copy(k.at[:, lanes(y, 128)], kvx.at[0, 0, :, pl.ds(0, 128)], lsem.at[0])
    own_v = pltpu.make_async_copy(v.at[:, lanes(y, 128)], kvx.at[0, 0, :, pl.ds(128, 128)], lsem.at[1])
    own_k.start()
    own_v.start()
    kv, rest = [], []
    for d in (2, 1, 3):
        t, dev = (y + d) % 4, along[d - 1]
        kv.append(remote(k.at[:, lanes(t, 128)], kvx.at[0, d, :, pl.ds(0, 128)], ssem.at[0, d], rsem.at[0, d], dev))
        kv.append(remote(v.at[:, lanes(t, 128)], kvx.at[0, d, :, pl.ds(128, 128)], ssem.at[1, d], rsem.at[1, d], dev))
    for d in (2, 1, 3):
        t, dev = (y + d) % 4, along[d - 1]
        rest.append(remote(ld.at[t], ldx.at[d - 1], ssem.at[2, d], rsem.at[2, d], dev))
        rest.append(remote(q.at[:, lanes(t, 512)], qx.at[d - 1], ssem.at[3, d], rsem.at[3, d], dev))
        rest.append(remote(do.at[:, lanes(t, 512)], dox.at[d - 1], ssem.at[4, d], rsem.at[4, d], dev))
    own_k.wait()
    own_v.wait()
    for copy in kv:
        copy.wait_recv()
    far = remote(kvx.at[0], kvx.at[2], ssem.at[0, 0], rsem.at[0, 0], across)
    side = remote(kvx.at[0], kvx.at[1], ssem.at[1, 0], rsem.at[1, 0], partner)
    far.wait_recv()
    last = remote(kvx.at[2], kvx.at[3], ssem.at[2, 0], rsem.at[2, 0], partner)
    for copy in kv:
        copy.wait_send()
    for copy in rest:
        copy.wait()
    far.wait_send()
    side.wait()
    last.wait()


def attention_kernel(order, q, do, ld, qx, dox, ldx, kvx, dqx, dkv, ks, vs, kt, qs, dos, lds, dka, dva, dqt):
    b, s, xh, y, c = place()

    def stored(m, d):
        return seq_of(xh ^ (m >> 1), (y + 4 - d) % 4, c ^ (m & 1))

    def rows(block):
        return pl.ds(pl.multiple_of(block * 64, 64), 64)

    for m in range(4):
        for d in range(4):
            for half in range(2):
                to = rows(order[stored(m, d) * 2 + half])
                ks[to, :] = kvx[m, d, half * 64 : half * 64 + 64, 0:128]
                vs[to, :] = kvx[m, d, half * 64 : half * 64 + 64, 128:256]
    for n in range(8):
        kt[n] = ks[n * 256 : n * 256 + 256, :].T
    for d in range(4):
        for half in range(2):
            for h in range(4):
                at = (slice(half * 64, half * 64 + 64), slice(h * 128, h * 128 + 128))
                if d:
                    qs[d * 2 + half, h * 64 : h * 64 + 64, :] = qx[(d - 1, *at)]
                    dos[d * 2 + half, h * 64 : h * 64 + 64, :] = dox[(d - 1, *at)]
                else:
                    own = lanes(y * 4 + h, 128)
                    qs[half, h * 64 : h * 64 + 64, :] = q[half * 64 : half * 64 + 64, own]
                    dos[half, h * 64 : h * 64 + 64, :] = do[half * 64 : half * 64 + 64, own]
        lds[d] = ldx[d - 1] if d else ld[y]
    dka[...] = jnp.zeros_like(dka)
    dva[...] = jnp.zeros_like(dva)
    gap = (
        lax.broadcasted_iota(jnp.int32, (256, 256), 0)
        - lax.broadcasted_iota(jnp.int32, (256, 256), 1) % 64
    )

    def piece(d, i):
        first = order[stored(0, d) * 2]
        turn = first // 4 + 1
        half = jnp.where(i < turn, 0, 1)
        n = jnp.where(i < turn, i, i - turn)
        block = jnp.where(i < turn, first, 31 - first)
        keys = pl.ds(pl.multiple_of(n * 256, 256), 256)
        qb, dob = qs[d * 2 + half], dos[d * 2 + half]
        base = half * 4
        lse = jnp.concatenate([lds[d, pl.ds(base, 1), :], lds[d, pl.ds(base + 1, 1), :]], axis=1)
        delta = jnp.concatenate([lds[d, pl.ds(base + 2, 1), :], lds[d, pl.ds(base + 3, 1), :]], axis=1)
        nt = (((1,), (1,)), ((), ()))
        scores = lax.dot_general(ks[keys, :], qb, nt, preferred_element_type=F32)
        probs = jnp.exp2(scores * (SCALE * LOG2E) - lse)
        probs = jnp.where(gap <= block * 64 - n * 256, probs, 0.0)
        dprobs = lax.dot_general(vs[keys, :], dob, nt, preferred_element_type=F32)
        dscores = (probs * (dprobs - delta) * SCALE).astype(BF)
        low = probs.astype(BF)
        dva[keys, :] += jnp.dot(low, dob, preferred_element_type=F32)
        dka[keys, :] += jnp.dot(dscores, qb, preferred_element_type=F32)
        dqt[half] += jnp.dot(kt[n], dscores, preferred_element_type=F32)

    @pl.loop(0, 4)
    def _(d):
        dqt[...] = jnp.zeros_like(dqt)

        @pl.loop(0, 3)
        def _(t):
            for u in range(3):
                piece(d, t * 3 + u)

        for half in range(2):
            dq = dqt[half].T
            for h in range(4):
                dqx[d, half * 64 : half * 64 + 64, h * 128 : h * 128 + 128] = dq[h * 64 : h * 64 + 64, :].astype(BF)

    for m in range(4):
        for d in range(4):
            for half in range(2):
                at = rows(order[stored(m, d) * 2 + half])
                dkv[m, d, half * 64 : half * 64 + 64, 0:128] = dka[at, :]
                dkv[m, d, half * 64 : half * 64 + 64, 128:256] = dva[at, :]


def reduce_kernel(
    dkv, dqx, hid, dq, dk, dv, kw, vw,
    hx, ht, sa, ra, sx, rx, g, acc, sb, rb, sy, ry, sf, rf,
    ssem, rsem, xsem, ysem, fsend, frecv, lsem,
):
    b, s, xh, y, c = place()
    along, partner, across = near(b, xh, y, c)
    quarter = xh * 2 + c
    to_b = y * 4 + quarter
    from_s = seq_of((b % 4) // 2, b // 4, b % 2)
    mine = to_b == b

    barrier = pltpu.get_barrier_semaphore()
    for dev in (*along, partner, across):
        signal(barrier, dev)

    @pl.loop(0, 16)
    def _(i):
        @pl.when(jnp.logical_not(mine & (i == s)))
        def _():
            signal(barrier, (to_b, i))

        @pl.when(jnp.logical_not(mine & (i == b)))
        def _():
            signal(barrier, (i, from_s))

    pl.semaphore_wait(barrier, jnp.where(mine, 35, 37))

    own_h = pltpu.make_async_copy(hid.at[:, lanes(y, 512)], hx.at[0], lsem.at[0])
    own_q = pltpu.make_async_copy(dqx.at[0], dq.at[:, lanes(y, 512)], lsem.at[1])
    own_h.start()
    own_q.start()
    home, feats = [], []
    for d in (2, 1, 3):
        dev = along[d - 1]
        feats.append(remote(hid.at[:, lanes((y + d) % 4, 512)], hx.at[d], ssem.at[0, d], rsem.at[0, d], dev))
    for d in (2, 1, 3):
        dev = along[(4 - d) - 1]
        home.append(remote(dqx.at[d], dq.at[:, lanes(y, 512)], ssem.at[1, d], rsem.at[1, d], dev))

    def summed(part, send, recv, send_far, recv_far, sems):
        send[1] = part(3).astype(BF)
        one = remote(send.at[1], recv.at[1], sems.at[0, 0], sems.at[0, 1], partner)
        send[0] = part(1).astype(BF)
        two = remote(send.at[0], recv.at[0], sems.at[1, 0], sems.at[1, 1], partner)
        one.wait_recv()
        send_far[...] = (part(2) + recv[1].astype(F32)).astype(BF)
        far = remote(send_far, recv_far, sems.at[2, 0], sems.at[2, 1], across)
        two.wait_recv()
        far.wait_recv()
        total = part(0) + recv[0].astype(F32) + recv_far[...].astype(F32)
        one.wait_send()
        two.wait_send()
        far.wait_send()
        return total

    g[0] = summed(lambda m: dkv[m], sa, ra, sx, rx, xsem).astype(BF)
    grads = {}
    for e in (2, 1, 3):
        grads[e] = remote(g.at[0], g.at[e], ssem.at[2, e], rsem.at[2, e], along[e - 1])
    own_h.wait()
    for copy in feats:
        copy.wait()
    for d in range(4):
        ht[:, d * 128 : d * 128 + 128] = hx[d].T
    for e in (0, 1, 3, 2):
        if e:
            grads[e].wait_recv()
        head = (y + 4 - e) % 4
        own = (4 - e) % 4
        dk[:, lanes(head, 128)] = g[e, own, :, 0:128]
        dv[:, lanes(head, 128)] = g[e, own, :, 128:256]
        tokens = jnp.concatenate([g[e, (d + 4 - e) % 4] for d in range(4)], axis=0)
        acc[:, lanes(head, 256)] = jnp.dot(ht[...], tokens, preferred_element_type=F32)

    def quarter_rows(m):
        at = (xh ^ (m >> 1)) * 2 + (c ^ (m & 1))
        return acc[pl.ds(pl.multiple_of(at * 128, 128), 128), :]

    total = summed(quarter_rows, sb, rb, sy, ry, ysem)
    sf[...] = total.reshape(16, 8, 1024).astype(BF)

    @pl.loop(0, 16)
    def _(i):
        is_me = mine & (i == s)

        @pl.when(is_me)
        def _():
            pltpu.make_async_copy(sf.at[i], rf.at[b], lsem.at[2]).start()

        @pl.when(jnp.logical_not(is_me))
        def _():
            remote(sf.at[i], rf.at[b], fsend.at[i], frecv.at[b], (to_b, i))

    @pl.loop(0, 16)
    def _(i):
        is_me = mine & (i == b)

        @pl.when(is_me)
        def _():
            pltpu.make_async_copy(sf.at[s], rf.at[i], lsem.at[2]).wait()

        @pl.when(jnp.logical_not(is_me))
        def _():
            pltpu.make_async_remote_copy(
                src_ref=sf.at[0], dst_ref=rf.at[i], send_sem=fsend.at[0], recv_sem=frecv.at[i],
                device_id=(i, from_s), device_id_type=MESH,
            ).wait_recv()

    rows = jnp.sum(rf[...].astype(F32), axis=0)
    for h in range(4):
        kw[:, h * 128 : h * 128 + 128] = rows[:, h * 256 : h * 256 + 128]
        vw[:, h * 128 : h * 128 + 128] = rows[:, h * 256 + 128 : h * 256 + 256]

    @pl.loop(0, 16)
    def _(i):
        @pl.when(jnp.logical_not(mine & (i == s)))
        def _():
            pltpu.make_async_remote_copy(
                src_ref=sf.at[i], dst_ref=rf.at[b], send_sem=fsend.at[i], recv_sem=frecv.at[b],
                device_id=(to_b, i), device_id_type=MESH,
            ).wait_send()

    own_q.wait()
    for copy in home:
        copy.wait()
    for e in (1, 2, 3):
        grads[e].wait_send()


VMEM = pl.BlockSpec(memory_space=pltpu.VMEM)
SMEM = pl.BlockSpec(memory_space=pltpu.SMEM)
ANY = pl.BlockSpec(memory_space=pl.ANY)


def struct(shape, dtype):
    return jax.ShapeDtypeStruct(shape, dtype)


def shards(hidden_in, queries, key_states, value_states, grad_out, log_sums, deltas, block_order):
    hid, q, do = hidden_in[0], queries[0], grad_out[0]
    k, v = key_states[0], value_states[0]
    ld = jnp.stack([log_sums[0] * LOG2E, deltas[0]]).reshape(2, HK, 2, 2, 2, 64)
    ld = ld.transpose(1, 4, 0, 2, 3, 5).reshape(HK, 8, 128)
    DMA = pltpu.SemaphoreType.DMA
    qx, dox, kvx, ldx = pl.pallas_call(
        gather_kernel,
        out_shape=(
            struct((3, 128, 512), BF),
            struct((3, 128, 512), BF),
            struct((4, 4, 128, 256), BF),
            struct((3, 8, 128), F32),
        ),
        in_specs=[ANY, ANY, VMEM, VMEM, VMEM],
        out_specs=(ANY, ANY, VMEM, VMEM),
        scratch_shapes=[DMA((5, 4)), DMA((5, 4)), DMA((2,))],
        name="gather",
        compiler_params=pltpu.CompilerParams(collective_id=0, has_side_effects=True),
    )(q, do, k, v, ld)
    dqx, dkv = pl.pallas_call(
        attention_kernel,
        out_shape=(struct((4, 128, 512), BF), struct((4, 4, 128, 256), F32)),
        in_specs=[SMEM] + [VMEM] * 7,
        out_specs=(VMEM, VMEM),
        scratch_shapes=[
            pltpu.VMEM((2048, 128), BF),
            pltpu.VMEM((2048, 128), BF),
            pltpu.VMEM((8, 128, 256), BF),
            pltpu.VMEM((8, 256, 128), BF),
            pltpu.VMEM((8, 256, 128), BF),
            pltpu.VMEM((4, 8, 128), F32),
            pltpu.VMEM((2048, 128), F32),
            pltpu.VMEM((2048, 128), F32),
            pltpu.VMEM((2, 128, 256), F32),
        ],
        name="attention",
    )(block_order, q, do, ld, qx, dox, ldx, kvx)
    dq, dk, dv, kw, vw = pl.pallas_call(
        reduce_kernel,
        out_shape=(
            struct((128, 2048), BF),
            struct((128, 512), BF),
            struct((128, 512), BF),
            struct((8, 512), F32),
            struct((8, 512), F32),
        ),
        in_specs=[VMEM] * 3,
        out_specs=(VMEM,) * 5,
        scratch_shapes=[
            pltpu.VMEM((4, 128, 512), BF),
            pltpu.VMEM((512, 512), BF),
            pltpu.VMEM((2, 4, 128, 256), BF),
            pltpu.VMEM((2, 4, 128, 256), BF),
            pltpu.VMEM((4, 128, 256), BF),
            pltpu.VMEM((4, 128, 256), BF),
            pltpu.VMEM((4, 4, 128, 256), BF),
            pltpu.VMEM((512, 1024), F32),
            pltpu.VMEM((2, 128, 1024), BF),
            pltpu.VMEM((2, 128, 1024), BF),
            pltpu.VMEM((128, 1024), BF),
            pltpu.VMEM((128, 1024), BF),
            pltpu.VMEM((16, 8, 1024), BF),
            pltpu.VMEM((16, 8, 1024), BF),
            DMA((3, 4)),
            DMA((3, 4)),
            DMA((3, 2)),
            DMA((3, 2)),
            DMA((16,)),
            DMA((16,)),
            DMA((3,)),
        ],
        name="reduce",
        compiler_params=pltpu.CompilerParams(collective_id=1, has_side_effects=True),
    )(dkv, dqx, hid)
    return (dq[None], dk[None], dv[None], kw, vw)


def solution(mesh):
    tokens, rows = P("batch", "seq", None), P("batch", None, "seq")
    return jax.shard_map(
        shards,
        mesh=mesh,
        in_specs=(tokens, tokens, tokens, tokens, tokens, rows, rows, P()),
        out_specs=(tokens, tokens, tokens, P(("batch", "seq"), None), P(("batch", "seq"), None)),
        check_vma=False,
    )
```

```python
import math

import jax
import jax.numpy as jnp
from jax import lax
from jax.experimental import pallas as pl
from jax.experimental.pallas import tpu as pltpu
from jax.sharding import PartitionSpec as P

MESH = pl.DeviceIdType.MESH
DH = 128
SCALE = 1.0 / math.sqrt(DH)
LOG2E = math.log2(math.e)
BF = jnp.bfloat16
F32 = jnp.float32
NT = (((1,), (1,)), ((), ()))


def place():
    b, s = lax.axis_index("batch"), lax.axis_index("seq")
    return b, s, s // 8, (s // 2) % 4, s % 2


def seq_of(xh, y, c):
    return xh * 8 + y * 2 + c


def remote_copy(src, dst, send, recv, dev):
    return pltpu.make_async_remote_copy(
        src_ref=src, dst_ref=dst, send_sem=send, recv_sem=recv, device_id=dev, device_id_type=MESH
    )


def remote(*args):
    copy = remote_copy(*args)
    copy.start()
    return copy


def lanes(index, width):
    return pl.ds(pl.multiple_of(index * width, width), width)


def fused_kernel(
    order, q, do, k, v, lse, dl, hid_in, dqh, kvg, wout,
    hid, qx, dox, kvx, lx, dx, hts, ht, ks, vs, kt, qs, dos, lsv, dlv, dka, dva, dkw, dvw, ek, ev, dqt, dqx,
    sa, ra, sx, rx, gg, acc, sb, rb, sy, ry, sf, rf, wsum,
    ssem, rsem, xsem, ysem, fsend, frecv, lsem,
):
    b, s, xh, y, c = place()
    along = [None] + [(b, seq_of(xh, (y + d) % 4, c)) for d in (1, 2, 3)]
    partner, across = (b, seq_of(xh, y, 1 - c)), (b, seq_of(1 - xh, y, c))

    own = [
        pltpu.make_async_copy(k.at[:, :, lanes(y, 128)], kvx.at[pl.ds(0, 2), :, pl.ds(0, 128)], lsem.at[0]),
        pltpu.make_async_copy(v.at[:, :, lanes(y, 128)], kvx.at[pl.ds(0, 2), :, pl.ds(128, 128)], lsem.at[1]),
        pltpu.make_async_copy(q.at[:, lanes(y, 512)], qx.at[0], lsem.at[2]),
        pltpu.make_async_copy(do.at[:, lanes(y, 512)], dox.at[0], lsem.at[3]),
        pltpu.make_async_copy(lse.at[y], lx.at[0], lsem.at[4]),
        pltpu.make_async_copy(dl.at[y], dx.at[0], lsem.at[5]),
    ]
    load = pltpu.make_async_copy(hid_in, hid, lsem.at[6])
    for copy in own:
        copy.start()
    load.start()

    barrier = pltpu.get_barrier_semaphore()
    for dev in (*along[1:], partner, across):
        pl.semaphore_signal(barrier, inc=1, device_id=dev, device_id_type=MESH)

    @pl.loop(1, 16)
    def _(t):
        pl.semaphore_signal(barrier, inc=1, device_id=((b + t) % 16, s), device_id_type=MESH)

    pl.semaphore_wait(barrier, 20)

    kv = []
    for d in (2, 1, 3):
        t, to = (y + d) % 4, pl.ds(2 * d, 2)
        kv.append(remote(k.at[:, :, lanes(t, 128)], kvx.at[to, :, pl.ds(0, 128)], ssem.at[0, d], rsem.at[0, d], along[d]))
        kv.append(remote(v.at[:, :, lanes(t, 128)], kvx.at[to, :, pl.ds(128, 128)], ssem.at[1, d], rsem.at[1, d], along[d]))
    rows_in = {}
    for d in (1, 3, 2):
        t = (y + d) % 4
        rows_in[d] = [
            remote(lse.at[t], lx.at[d], ssem.at[2, d], rsem.at[2, d], along[d]),
            remote(dl.at[t], dx.at[d], ssem.at[3, d], rsem.at[3, d], along[d]),
            remote(q.at[:, lanes(t, 512)], qx.at[d], ssem.at[4, d], rsem.at[4, d], along[d]),
            remote(do.at[:, lanes(t, 512)], dox.at[d], ssem.at[5, d], rsem.at[5, d], along[d]),
        ]

    load.wait()
    row = lax.broadcasted_iota(jnp.int32, (128, 128), 0)
    col = lax.broadcasted_iota(jnp.int32, (128, 128), 1)
    wanted = (row // 64) * 64 + ((row // 8) % 4) * 16 + ((row // 32) % 2) * 8 + row % 8
    pick = jnp.where(col == wanted, 1.0, 0.0).astype(BF)
    for i in range(16):
        turned = lax.dot_general(pick, hid[:, i * 128 : i * 128 + 128], NT, preferred_element_type=F32).astype(BF)
        for p in range(4):
            hts[p * 512 + i * 32 : p * 512 + i * 32 + 32, :] = turned[p * 32 : p * 32 + 32, :]
    feats = {}
    for d in (1, 3, 2):
        feats[d] = remote(hts, ht.at[:, pl.ds(d * 128, 128)], ssem.at[6, d], rsem.at[6, d], along[d])
    ht[:, 0:128] = hts[...]

    for copy in own:
        copy.wait()
    for copy in kv:
        copy.wait_recv()
    far = remote(kvx.at[pl.ds(0, 8)], kvx.at[pl.ds(16, 8)], ssem.at[0, 0], rsem.at[0, 0], across)
    side = remote(kvx.at[pl.ds(0, 8)], kvx.at[pl.ds(8, 8)], ssem.at[1, 0], rsem.at[1, 0], partner)
    slot_of = [None] * 32
    firsts = [order[2 * i] for i in range(16)]
    for n in range(16):
        code = jnp.int32(0)
        for i in range(16):
            code = jnp.where(firsts[i] == n, 2 * i, jnp.where(firsts[i] == 31 - n, 2 * i + 1, code))
        pair, flip = code // 2, code % 2
        index = (((pair // 8) ^ xh) * 2 + ((pair % 2) ^ c)) * 8 + ((y + 4 - (pair // 2) % 4) % 4) * 2
        slot_of[n], slot_of[31 - n] = index + flip, index + 1 - flip
    far.wait_recv()
    last = remote(kvx.at[pl.ds(16, 8)], kvx.at[pl.ds(24, 8)], ssem.at[2, 0], rsem.at[2, 0], partner)
    gap = (
        lax.broadcasted_iota(jnp.int32, (256, 256), 0)
        - lax.broadcasted_iota(jnp.int32, (256, 256), 1) % 64
    )
    dka[0:1024, :] = jnp.zeros((1024, 128), F32)
    dva[0:1024, :] = jnp.zeros((1024, 128), F32)
    side.wait_recv()
    last.wait_recv()
    for n in range(32):
        both = kvx[slot_of[n]]
        ks[n // 4, n % 4 * 64 : n % 4 * 64 + 64, :] = both[:, 0:128]
        vs[n // 4, n % 4 * 64 : n % 4 * 64 + 64, :] = both[:, 128:256]
    for n in range(8):
        kt[n] = ks[n].T

    def first_of(d):
        return order[seq_of(xh, (y + 4 - d) % 4, c) * 2]

    def low_of(d):
        first = first_of(d)
        return jnp.minimum(first, 31 - first)

    def piece(h, n, block):
        scores = lax.dot_general(ks[n], qs[h], NT, preferred_element_type=F32)
        probs = jnp.exp2(scores * (SCALE * LOG2E) - lsv[h])
        if block is not None:
            probs = jnp.where(gap <= block * 64 - n * 256, probs, 0.0)
        dprobs = lax.dot_general(vs[n], dos[h], NT, preferred_element_type=F32)
        dscores = (probs * (dprobs - dlv[h]) * SCALE).astype(BF)
        return (
            jnp.dot(dscores, qs[h], preferred_element_type=F32),
            jnp.dot(probs.astype(BF), dos[h], preferred_element_type=F32),
            jnp.dot(kt[n], dscores, preferred_element_type=F32),
        )

    def home_copy(d):
        dev = (b, seq_of(xh, (y + 4 - d) % 4, c))
        return remote_copy(dqx.at[d], dqh.at[:, lanes(y, 512)], ssem.at[7, d], rsem.at[7, d], dev)

    lane = lax.broadcasted_iota(jnp.int32, (1, 128), 1) < 64

    @pl.loop(0, 4)
    def _(turn):
        d = jnp.where(turn == 2, 3, jnp.where(turn == 3, 2, turn))

        @pl.when(turn > 0)
        def _():
            dev = (b, seq_of(xh, (y + 4 - d) % 4, c))
            remote_copy(lse.at[0], lx.at[d], ssem.at[2, d], rsem.at[2, d], dev).wait_recv()
            remote_copy(dl.at[0], dx.at[d], ssem.at[3, d], rsem.at[3, d], dev).wait_recv()
            remote_copy(q.at[:, pl.ds(0, 512)], qx.at[d], ssem.at[4, d], rsem.at[4, d], dev).wait_recv()
            remote_copy(do.at[:, pl.ds(0, 512)], dox.at[d], ssem.at[5, d], rsem.at[5, d], dev).wait_recv()

        flip = first_of(d) >= 16
        low = low_of(d)
        quad = low // 4
        for source, target in ((qx, qs), (dox, dos)):
            for h in range(4):
                zero = source[d, 0:64, h * 128 : h * 128 + 128]
                one = source[d, 64:128, h * 128 : h * 128 + 128]
                target[0, h * 64 : h * 64 + 64, :] = jnp.where(flip, one, zero)
                target[1, h * 64 : h * 64 + 64, :] = jnp.where(flip, zero, one)
        for source, target, factor in ((lx, lsv, LOG2E), (dx, dlv, None)):
            plain = source[d]
            rolled = pltpu.roll(plain, 64, axis=1)
            pairs = []
            for left, right in ((plain, rolled), (rolled, plain)):
                line = jnp.concatenate(
                    [jnp.where(lane, left[h : h + 1, :], right[h + 1 : h + 2, :]) for h in (0, 2)], axis=1
                )
                pairs.append(line if factor is None else line * factor)
            target[0] = jnp.where(flip, pairs[1], pairs[0])
            target[1] = jnp.where(flip, pairs[0], pairs[1])
        dqt[...] = jnp.zeros_like(dqt)
        for n in range(4):
            dk, dv, dq = piece(1, n, None)
            dka[n * 256 : n * 256 + 256, :] += dk
            dva[n * 256 : n * 256 + 256, :] += dv
            dqt[1] += dq
        for j in range(4):
            is_low = j <= quad
            dk, dv, dq = piece(
                jnp.where(is_low, 0, 1), jnp.where(is_low, j, 7 - j), jnp.where(is_low, low, 31 - low)
            )
            ek[d * 5 + j] = dk
            ev[d * 5 + j] = dv
            dqt[0] += jnp.where(is_low, dq, 0.0)
            dqt[1] += jnp.where(is_low, 0.0, dq)
        dk, dv, dq = piece(1, 7 - quad, 31 - low)
        ek[d * 5 + 4] = dk
        ev[d * 5 + 4] = dv
        dqt[1] += dq
        low_q, high_q = dqt[0].T, dqt[1].T
        for h in range(4):
            lo, hi = low_q[h * 64 : h * 64 + 64, :].astype(BF), high_q[h * 64 : h * 64 + 64, :].astype(BF)
            dqx[d, 0:64, h * 128 : h * 128 + 128] = jnp.where(flip, hi, lo)
            dqx[d, 64:128, h * 128 : h * 128 + 128] = jnp.where(flip, lo, hi)

        @pl.when(turn > 0)
        def _():
            home_copy(d).start()

    own_q = pltpu.make_async_copy(dqx.at[0], dqh.at[:, lanes(y, 512)], lsem.at[0])
    own_q.start()
    quads = [low_of(d) // 4 for d in range(4)]

    @pl.loop(0, 4)
    def _(part):
        for n in range(8):
            at = pl.ds(pl.multiple_of(n * 256 + part * 64, 64), 64)
            sub = pl.ds(pl.multiple_of(part * 64, 64), 64)
            for store, extra, whole in ((dka, ek, dkw), (dva, ev, dvw)):
                total = store[at, :] if n < 4 else jnp.zeros((64, 128), F32)
                for d in range(4):
                    if n < 4:
                        total += jnp.where(n <= quads[d], extra[d * 5 + n, sub, :], 0.0)
                    else:
                        total += jnp.where(7 - n > quads[d], extra[d * 5 + 7 - n, sub, :], 0.0)
                        total += jnp.where(7 - n == quads[d], extra[d * 5 + 4, sub, :], 0.0)
                whole[n * 4 + part] = total

    def summed(part, put, send, recv, send_far, recv_far, sems):
        blocks = [slice(i * 64, i * 64 + 64) for i in range(8)]
        for i in range(8):
            send[1, blocks[i], :] = part(3, i).astype(BF)
        one = remote(send.at[1], recv.at[1], sems.at[0, 0], sems.at[0, 1], partner)
        for i in range(8):
            send[0, blocks[i], :] = part(1, i).astype(BF)
        two = remote(send.at[0], recv.at[0], sems.at[1, 0], sems.at[1, 1], partner)
        one.wait_recv()
        for i in range(8):
            send_far[blocks[i], :] = (part(2, i) + recv[1, blocks[i], :].astype(F32)).astype(BF)
        far = remote(send_far, recv_far, sems.at[2, 0], sems.at[2, 1], across)
        two.wait_recv()
        far.wait_recv()
        for i in range(8):
            put(i, part(0, i) + recv[0, blocks[i], :].astype(F32) + recv_far[blocks[i], :].astype(F32))
        return one, two, far

    def grads_part(m, i):
        block = order[seq_of(xh ^ (m >> 1), (y + 4 - i // 2) % 4, c ^ (m & 1)) * 2 + i % 2]
        return jnp.concatenate([dkw[block], dvw[block]], axis=1)

    def put_grads(i, value):
        gg[i * 64 : i * 64 + 64, :] = value.astype(BF)

    sent = list(summed(grads_part, put_grads, sa, ra, sx, rx, xsem))
    back = []
    for d in (1, 2, 3):
        back.append(remote(gg.at[pl.ds(d * 128, 128)], kvg.at[d], ssem.at[8, d], rsem.at[8, d], along[4 - d]))
    own_g = pltpu.make_async_copy(gg.at[pl.ds(0, 128)], kvg.at[0], lsem.at[1])
    own_g.start()
    for d in (1, 3, 2):
        feats[d].wait_recv()
    for m in (3, 1, 2, 0):
        at = (xh ^ (m >> 1)) * 2 + (c ^ (m & 1))
        rows = pl.ds(pl.multiple_of(at * 512, 512), 512)
        acc[m] = jnp.dot(ht[rows, :], gg[...], preferred_element_type=F32)

    def put_rows(i, value):
        sf[2 * i] = value[0:32, :].astype(BF)
        sf[2 * i + 1] = value[32:64, :].astype(BF)

    sent += summed(lambda m, i: acc[m, i * 64 : i * 64 + 64, :], put_rows, sb, rb, sy, ry, ysem)

    def batch_copy(t):
        to = (b + t) % 16
        return remote_copy(sf.at[to], rf.at[t], fsend.at[t], frecv.at[t], (to, s))

    @pl.loop(1, 16)
    def _(t):
        batch_copy(t).start()

    rf[0] = sf[b]

    @pl.loop(1, 16)
    def _(t):
        batch_copy(t).wait_recv()

    total = jnp.sum(rf[...].astype(F32), axis=0)
    for t in range(4):
        wsum[t] = total[t * 8 : t * 8 + 8, :]
    tail = [remote(wsum.at[(y + d) % 4], wout.at[d], ssem.at[9, d], rsem.at[9, d], along[d]) for d in (1, 2, 3)]
    own_w = pltpu.make_async_copy(wsum.at[y], wout.at[0], lsem.at[2])
    own_w.start()

    @pl.loop(1, 16)
    def _(t):
        batch_copy(t).wait_send()

    for copy in (own_q, own_g, own_w):
        copy.wait()
    for d in (1, 2, 3):
        home_copy(d).wait()
        feats[d].wait_send()
        for copy in rows_in[d]:
            copy.wait_send()
    for copy in (*kv, far, side, *sent):
        copy.wait_send()
    last.wait_send()
    for copy in (*back, *tail):
        copy.wait()


def finish_kernel(dqh, kvg, wout, dq, dk, dv, kw, vw):
    _, _, _, y, _ = place()
    dq[...] = dqh[...]
    for d in range(4):
        head = lanes((y + d) % 4, 128)
        dk[:, head] = kvg[d, :, 0:128]
        dv[:, head] = kvg[d, :, 128:256]
        head = lanes((y + 4 - d) % 4, 128)
        kw[:, head] = wout[d, :, 0:128]
        vw[:, head] = wout[d, :, 128:256]


VMEM = pl.BlockSpec(memory_space=pltpu.VMEM)
SMEM = pl.BlockSpec(memory_space=pltpu.SMEM)
ANY = pl.BlockSpec(memory_space=pl.ANY)


def struct(shape, dtype):
    return jax.ShapeDtypeStruct(shape, dtype)


def shards(hidden_in, queries, key_states, value_states, grad_out, log_sums, deltas, block_order):
    DMA = pltpu.SemaphoreType.DMA
    dqh, kvg, wout = pl.pallas_call(
        fused_kernel,
        out_shape=(struct((128, 2048), BF), struct((4, 128, 256), BF), struct((4, 8, 256), F32)),
        in_specs=[SMEM] + [ANY] * 7,
        out_specs=(ANY,) * 3,
        scratch_shapes=[
            pltpu.VMEM((128, 2048), BF),
            pltpu.VMEM((4, 128, 512), BF),
            pltpu.VMEM((4, 128, 512), BF),
            pltpu.VMEM((32, 64, 256), BF),
            pltpu.VMEM((4, 4, 128), F32),
            pltpu.VMEM((4, 4, 128), F32),
            pltpu.VMEM((2048, 128), BF),
            pltpu.VMEM((2048, 512), BF),
            pltpu.VMEM((8, 256, 128), BF),
            pltpu.VMEM((8, 256, 128), BF),
            pltpu.VMEM((8, 128, 256), BF),
            pltpu.VMEM((2, 256, 128), BF),
            pltpu.VMEM((2, 256, 128), BF),
            pltpu.VMEM((2, 1, 256), F32),
            pltpu.VMEM((2, 1, 256), F32),
            pltpu.VMEM((1024, 128), F32),
            pltpu.VMEM((1024, 128), F32),
            pltpu.VMEM((32, 64, 128), F32),
            pltpu.VMEM((32, 64, 128), F32),
            pltpu.VMEM((20, 256, 128), F32),
            pltpu.VMEM((20, 256, 128), F32),
            pltpu.VMEM((2, 128, 256), F32),
            pltpu.VMEM((4, 128, 512), BF),
            pltpu.VMEM((2, 512, 256), BF),
            pltpu.VMEM((2, 512, 256), BF),
            pltpu.VMEM((512, 256), BF),
            pltpu.VMEM((512, 256), BF),
            pltpu.VMEM((512, 256), BF),
            pltpu.VMEM((4, 512, 256), F32),
            pltpu.VMEM((2, 512, 256), BF),
            pltpu.VMEM((2, 512, 256), BF),
            pltpu.VMEM((512, 256), BF),
            pltpu.VMEM((512, 256), BF),
            pltpu.VMEM((16, 32, 256), BF),
            pltpu.VMEM((16, 32, 256), BF),
            pltpu.VMEM((4, 8, 256), F32),
            DMA((10, 4)),
            DMA((10, 4)),
            DMA((3, 2)),
            DMA((3, 2)),
            DMA((16,)),
            DMA((16,)),
            DMA((7,)),
        ],
        name="fused",
        compiler_params=pltpu.CompilerParams(collective_id=0, has_side_effects=True),
    )(
        block_order,
        queries[0],
        grad_out[0],
        key_states.reshape(2, 64, 512),
        value_states.reshape(2, 64, 512),
        log_sums.reshape(4, 4, 128),
        deltas.reshape(4, 4, 128),
        hidden_in[0],
    )
    dq, dk, dv, kw, vw = pl.pallas_call(
        finish_kernel,
        out_shape=(
            struct((128, 2048), BF),
            struct((128, 512), BF),
            struct((128, 512), BF),
            struct((8, 512), F32),
            struct((8, 512), F32),
        ),
        in_specs=[VMEM] * 3,
        out_specs=(VMEM,) * 5,
        name="finish",
    )(dqh, kvg, wout)
    return (dq[None], dk[None], dv[None], kw, vw)


def solution(mesh):
    tokens, rows = P("batch", "seq", None), P("batch", None, "seq")
    return jax.shard_map(
        shards,
        mesh=mesh,
        in_specs=(tokens, tokens, tokens, tokens, tokens, rows, rows, P()),
        out_specs=(tokens, tokens, tokens, P(("batch", "seq"), None), P(("batch", "seq"), None)),
        check_vma=False,
    )
```

```python
import math

import jax
import jax.numpy as jnp
from jax import lax
from jax.experimental import pallas as pl
from jax.experimental.pallas import tpu as pltpu
from jax.sharding import PartitionSpec as P

MESH = pl.DeviceIdType.MESH
DH = 128
SCALE = 1.0 / math.sqrt(DH)
LOG2E = math.log2(math.e)
BF = jnp.bfloat16
F32 = jnp.float32
NT = (((1,), (1,)), ((), ()))


def place():
    b, s = lax.axis_index("batch"), lax.axis_index("seq")
    return b, s, s // 8, (s // 2) % 4, s % 2


def seq_of(xh, y, c):
    return xh * 8 + y * 2 + c


def remote_copy(src, dst, send, recv, dev):
    return pltpu.make_async_remote_copy(
        src_ref=src, dst_ref=dst, send_sem=send, recv_sem=recv, device_id=dev, device_id_type=MESH
    )


def remote(*args):
    copy = remote_copy(*args)
    copy.start()
    return copy


def lanes(index, width):
    return pl.ds(pl.multiple_of(index * width, width), width)


def fused_kernel(
    order, q, do, k_in, v_in, lse, dl, hid_in, dqh, kvg, wout,
    hid, k, v, qx, dox, kvx, lx, dx, ht, ks, vs, kt, qs, dos, lsv, dlv, dka, dva, dkw, dvw, ek, ev, dqt, dqx,
    sa, ra, sx, rx, gg, acc, sb, rb, sy, ry, sf, rf, wsum,
    ssem, rsem, xsem, ysem, fsend, frecv, lsem,
):
    b, s, xh, y, c = place()
    along = [None] + [(b, seq_of(xh, (y + d) % 4, c)) for d in (1, 2, 3)]
    partner, across = (b, seq_of(xh, y, 1 - c)), (b, seq_of(1 - xh, y, c))

    keys_in = pltpu.make_async_copy(k_in, k, lsem.at[7])
    values_in = pltpu.make_async_copy(v_in, v, lsem.at[8])
    keys_in.start()
    values_in.start()
    own = [
        pltpu.make_async_copy(k_in.at[:, :, lanes(y, 128)], kvx.at[pl.ds(0, 2), :, pl.ds(0, 128)], lsem.at[0]),
        pltpu.make_async_copy(v_in.at[:, :, lanes(y, 128)], kvx.at[pl.ds(0, 2), :, pl.ds(128, 128)], lsem.at[1]),
        pltpu.make_async_copy(q.at[:, lanes(y, 512)], qx.at[0], lsem.at[2]),
        pltpu.make_async_copy(do.at[:, lanes(y, 512)], dox.at[0], lsem.at[3]),
        pltpu.make_async_copy(lse.at[y], lx.at[0], lsem.at[4]),
        pltpu.make_async_copy(dl.at[y], dx.at[0], lsem.at[5]),
    ]
    load = pltpu.make_async_copy(hid_in, hid, lsem.at[6])
    for copy in own:
        copy.start()
    load.start()

    barrier = pltpu.get_barrier_semaphore()
    for dev in (*along[1:], partner, across):
        pl.semaphore_signal(barrier, inc=1, device_id=dev, device_id_type=MESH)

    @pl.loop(1, 16)
    def _(t):
        pl.semaphore_signal(barrier, inc=1, device_id=((b + t) % 16, s), device_id_type=MESH)

    pl.semaphore_wait(barrier, 20)

    keys_in.wait()
    values_in.wait()
    kv = [[], []]
    for part, (source, half) in enumerate(((k, pl.ds(0, 128)), (v, pl.ds(128, 128)))):
        for d in (2, 1, 3):
            from_, to = source.at[:, :, lanes((y + d) % 4, 128)], kvx.at[pl.ds(2 * d, 2), :, half]
            kv[part].append(remote(from_, to, ssem.at[part, d], rsem.at[part, d], along[d]))
    rows_in = {}
    for d in (1, 3, 2):
        t = (y + d) % 4
        rows_in[d] = [
            remote(lse.at[t], lx.at[d], ssem.at[2, d], rsem.at[2, d], along[d]),
            remote(dl.at[t], dx.at[d], ssem.at[3, d], rsem.at[3, d], along[d]),
            remote(q.at[:, lanes(t, 512)], qx.at[d], ssem.at[4, d], rsem.at[4, d], along[d]),
            remote(do.at[:, lanes(t, 512)], dox.at[d], ssem.at[5, d], rsem.at[5, d], along[d]),
        ]

    load.wait()
    row = lax.broadcasted_iota(jnp.int32, (128, 128), 0)
    col = lax.broadcasted_iota(jnp.int32, (128, 128), 1)
    wanted = (row // 64) * 64 + ((row // 8) % 4) * 16 + ((row // 32) % 2) * 8 + row % 8
    pick = jnp.where(col == wanted, 1.0, 0.0).astype(BF)
    for i in range(16):
        turned = lax.dot_general(pick, hid[:, i * 128 : i * 128 + 128], NT, preferred_element_type=F32).astype(BF)
        for p in range(4):
            ht[0, p * 512 + i * 32 : p * 512 + i * 32 + 32, :] = turned[p * 32 : p * 32 + 32, :]
    feats = {}
    for d in (1, 3):
        feats[d] = remote(ht.at[0], ht.at[d], ssem.at[6, d], rsem.at[6, d], along[d])

    for copy in own:
        copy.wait()
    far, side = [], []
    for part in range(2):
        for copy in kv[part]:
            copy.wait_recv()
        half = pl.ds(part * 128, 128)
        mine, theirs = kvx.at[pl.ds(0, 8), :, half], kvx.at[pl.ds(16, 8), :, half]
        far.append(remote(mine, theirs, ssem.at[part, 0], rsem.at[part, 0], across))
        theirs = kvx.at[pl.ds(8, 8), :, half]
        side.append(remote(mine, theirs, ssem.at[2 + part, 0], rsem.at[2 + part, 0], partner))
    slot_of = [None] * 32
    firsts = [order[2 * i] for i in range(16)]
    for n in range(16):
        code = jnp.int32(0)
        for i in range(16):
            code = jnp.where(firsts[i] == n, 2 * i, jnp.where(firsts[i] == 31 - n, 2 * i + 1, code))
        pair, flip = code // 2, code % 2
        index = (((pair // 8) ^ xh) * 2 + ((pair % 2) ^ c)) * 8 + ((y + 4 - (pair // 2) % 4) % 4) * 2
        slot_of[n], slot_of[31 - n] = index + flip, index + 1 - flip
    gap = (
        lax.broadcasted_iota(jnp.int32, (256, 256), 0)
        - lax.broadcasted_iota(jnp.int32, (256, 256), 1) % 64
    )
    dka[0:1024, :] = jnp.zeros((1024, 128), F32)
    dva[0:1024, :] = jnp.zeros((1024, 128), F32)
    last = []
    for part in range(2):
        far[part].wait_recv()
        half = pl.ds(part * 128, 128)
        mine, theirs = kvx.at[pl.ds(16, 8), :, half], kvx.at[pl.ds(24, 8), :, half]
        last.append(remote(mine, theirs, ssem.at[4 + part, 0], rsem.at[4 + part, 0], partner))
    for copy in (*side, *last):
        copy.wait_recv()
    for n in range(32):
        both = kvx[slot_of[n]]
        ks[n // 4, n % 4 * 64 : n % 4 * 64 + 64, :] = both[:, 0:128]
        vs[n // 4, n % 4 * 64 : n % 4 * 64 + 64, :] = both[:, 128:256]
    for n in range(8):
        kt[n] = ks[n].T

    def first_of(d):
        return order[seq_of(xh, (y + 4 - d) % 4, c) * 2]

    def low_of(d):
        first = first_of(d)
        return jnp.minimum(first, 31 - first)

    def piece(h, n, block):
        scores = lax.dot_general(ks[n], qs[h], NT, preferred_element_type=F32)
        probs = jnp.exp2(scores * (SCALE * LOG2E) - lsv[h])
        if block is not None:
            probs = jnp.where(gap <= block * 64 - n * 256, probs, 0.0)
        dprobs = lax.dot_general(vs[n], dos[h], NT, preferred_element_type=F32)
        dscores = (probs * (dprobs - dlv[h]) * SCALE).astype(BF)
        return (
            jnp.dot(dscores, qs[h], preferred_element_type=F32),
            jnp.dot(probs.astype(BF), dos[h], preferred_element_type=F32),
            jnp.dot(kt[n], dscores, preferred_element_type=F32),
        )

    def home_copy(d):
        dev = (b, seq_of(xh, (y + 4 - d) % 4, c))
        return remote_copy(dqx.at[d], dqh.at[:, lanes(y, 512)], ssem.at[7, d], rsem.at[7, d], dev)

    lane = lax.broadcasted_iota(jnp.int32, (1, 128), 1) < 64

    @pl.loop(0, 4)
    def _(turn):
        d = jnp.where(turn == 2, 3, jnp.where(turn == 3, 2, turn))

        @pl.when(turn > 0)
        def _():
            dev = (b, seq_of(xh, (y + 4 - d) % 4, c))
            remote_copy(lse.at[0], lx.at[d], ssem.at[2, d], rsem.at[2, d], dev).wait_recv()
            remote_copy(dl.at[0], dx.at[d], ssem.at[3, d], rsem.at[3, d], dev).wait_recv()
            remote_copy(q.at[:, pl.ds(0, 512)], qx.at[d], ssem.at[4, d], rsem.at[4, d], dev).wait_recv()
            remote_copy(do.at[:, pl.ds(0, 512)], dox.at[d], ssem.at[5, d], rsem.at[5, d], dev).wait_recv()

        flip = first_of(d) >= 16
        low = low_of(d)
        quad = low // 4
        for source, target in ((qx, qs), (dox, dos)):
            for h in range(4):
                zero = source[d, 0:64, h * 128 : h * 128 + 128]
                one = source[d, 64:128, h * 128 : h * 128 + 128]
                target[0, h * 64 : h * 64 + 64, :] = jnp.where(flip, one, zero)
                target[1, h * 64 : h * 64 + 64, :] = jnp.where(flip, zero, one)
        for source, target, factor in ((lx, lsv, LOG2E), (dx, dlv, None)):
            plain = source[d]
            rolled = pltpu.roll(plain, 64, axis=1)
            pairs = []
            for left, right in ((plain, rolled), (rolled, plain)):
                line = jnp.concatenate(
                    [jnp.where(lane, left[h : h + 1, :], right[h + 1 : h + 2, :]) for h in (0, 2)], axis=1
                )
                pairs.append(line if factor is None else line * factor)
            target[0] = jnp.where(flip, pairs[1], pairs[0])
            target[1] = jnp.where(flip, pairs[0], pairs[1])
        dqt[...] = jnp.zeros_like(dqt)
        for n in range(4):
            dk, dv, dq = piece(1, n, None)
            dka[n * 256 : n * 256 + 256, :] += dk
            dva[n * 256 : n * 256 + 256, :] += dv
            dqt[1] += dq
        for j in range(4):
            is_low = j <= quad
            dk, dv, dq = piece(
                jnp.where(is_low, 0, 1), jnp.where(is_low, j, 7 - j), jnp.where(is_low, low, 31 - low)
            )
            ek[d * 5 + j] = dk
            ev[d * 5 + j] = dv
            dqt[0] += jnp.where(is_low, dq, 0.0)
            dqt[1] += jnp.where(is_low, 0.0, dq)
        dk, dv, dq = piece(1, 7 - quad, 31 - low)
        ek[d * 5 + 4] = dk
        ev[d * 5 + 4] = dv
        dqt[1] += dq
        low_q, high_q = dqt[0].T, dqt[1].T
        for h in range(4):
            lo, hi = low_q[h * 64 : h * 64 + 64, :].astype(BF), high_q[h * 64 : h * 64 + 64, :].astype(BF)
            dqx[d, 0:64, h * 128 : h * 128 + 128] = jnp.where(flip, hi, lo)
            dqx[d, 64:128, h * 128 : h * 128 + 128] = jnp.where(flip, lo, hi)

    own_q = pltpu.make_async_copy(dqx.at[0], dqh.at[:, lanes(y, 512)], lsem.at[0])
    own_q.start()
    quads = [low_of(d) // 4 for d in range(4)]

    @pl.loop(0, 4)
    def _(part):
        for n in range(8):
            at = pl.ds(pl.multiple_of(n * 256 + part * 64, 64), 64)
            sub = pl.ds(pl.multiple_of(part * 64, 64), 64)
            for store, extra, whole in ((dka, ek, dkw), (dva, ev, dvw)):
                total = store[at, :] if n < 4 else jnp.zeros((64, 128), F32)
                for d in range(4):
                    if n < 4:
                        total += jnp.where(n <= quads[d], extra[d * 5 + n, sub, :], 0.0)
                    else:
                        total += jnp.where(7 - n > quads[d], extra[d * 5 + 7 - n, sub, :], 0.0)
                        total += jnp.where(7 - n == quads[d], extra[d * 5 + 4, sub, :], 0.0)
                whole[n * 4 + part] = total

    def summed(part, put, after, send, recv, send_far, recv_far, sems):
        blocks = [slice(i * 64, i * 64 + 64) for i in range(8)]
        chunks = [(n, pl.ds(n * 256, 256), range(n * 4, n * 4 + 4)) for n in range(2)]
        one, two, far = [], [], []
        for n, rows, members in chunks:
            for i in members:
                send[1, blocks[i], :] = part(3, i).astype(BF)
            one.append(remote(send.at[1, rows], recv.at[1, rows], sems.at[0, 0, n], sems.at[0, 1, n], partner))
        for n, rows, members in chunks:
            for i in members:
                send[0, blocks[i], :] = part(1, i).astype(BF)
            two.append(remote(send.at[0, rows], recv.at[0, rows], sems.at[1, 0, n], sems.at[1, 1, n], partner))
        for n, rows, members in chunks:
            one[n].wait_recv()
            for i in members:
                send_far[blocks[i], :] = (part(2, i) + recv[1, blocks[i], :].astype(F32)).astype(BF)
            far.append(remote(send_far.at[rows], recv_far.at[rows], sems.at[2, 0, n], sems.at[2, 1, n], across))
        for n, rows, members in chunks:
            two[n].wait_recv()
            far[n].wait_recv()
            for i in members:
                put(i, part(0, i) + recv[0, blocks[i], :].astype(F32) + recv_far[blocks[i], :].astype(F32))
            after(n)
        return one + two + far

    def grads_part(m, i):
        block = order[seq_of(xh ^ (m >> 1), (y + 4 - i // 2) % 4, c ^ (m & 1)) * 2 + i % 2]
        return jnp.concatenate([dkw[block], dvw[block]], axis=1)

    def put_grads(i, value):
        gg[i * 64 : i * 64 + 64, :] = value.astype(BF)

    relays = []
    for d, to, half in ((1, 1, 0), (3, 3, 1)):
        feats[d].wait_recv()
        rows = pl.ds(half * 1024, 1024)
        relays.append(remote(ht.at[d, rows], ht.at[2, rows], ssem.at[6, 2 * half], rsem.at[6, 2 * half], along[to]))
    sent = summed(grads_part, put_grads, lambda n: None, sa, ra, sx, rx, xsem)
    back = []
    for d in (1, 2, 3):
        back.append(remote(gg.at[pl.ds(d * 128, 128)], kvg.at[d], ssem.at[8, d], rsem.at[8, d], along[4 - d]))
    own_g = pltpu.make_async_copy(gg.at[pl.ds(0, 128)], kvg.at[0], lsem.at[1])
    own_g.start()
    for copy in relays:
        copy.wait_recv()
    for d in (1, 3, 2):
        home_copy(d).start()
    for m in (3, 1, 2, 0):
        at = (xh ^ (m >> 1)) * 2 + (c ^ (m & 1))
        rows = pl.ds(pl.multiple_of(at * 512, 512), 512)
        acc[m] = jnp.dot(
            jnp.concatenate([ht[d, rows, :] for d in range(4)], axis=1), gg[...], preferred_element_type=F32
        )

    def put_rows(i, value):
        sf[2 * i] = value[0:32, :].astype(BF)
        sf[2 * i + 1] = value[32:64, :].astype(BF)

    def batch_copy(t):
        to = (b + t) % 16
        return remote_copy(sf.at[to], rf.at[t], fsend.at[t], frecv.at[t], (to, s))

    def spread(n):
        @pl.loop(n * 8, n * 8 + 8)
        def _(to):
            @pl.when(to != b)
            def _():
                batch_copy((to + 16 - b) % 16).start()

    sent += summed(lambda m, i: acc[m, i * 64 : i * 64 + 64, :], put_rows, spread, sb, rb, sy, ry, ysem)
    rf[0] = sf[b]

    @pl.loop(1, 16)
    def _(t):
        batch_copy(t).wait_recv()

    total = jnp.sum(rf[...].astype(F32), axis=0)
    for t in range(4):
        wsum[t] = total[t * 8 : t * 8 + 8, :]
    tail = [remote(wsum.at[(y + d) % 4], wout.at[d], ssem.at[9, d], rsem.at[9, d], along[d]) for d in (1, 2, 3)]
    own_w = pltpu.make_async_copy(wsum.at[y], wout.at[0], lsem.at[2])
    own_w.start()

    @pl.loop(1, 16)
    def _(t):
        batch_copy(t).wait_send()

    for copy in (own_q, own_g, own_w):
        copy.wait()
    for d in (1, 2, 3):
        home_copy(d).wait()
        for copy in rows_in[d]:
            copy.wait_send()
    for copy in (feats[1], feats[3], *relays, *kv[0], *kv[1], *far, *side, *last, *sent):
        copy.wait_send()
    for copy in (*back, *tail):
        copy.wait()


def finish_kernel(dqh, kvg, wout, dq, dk, dv, kw, vw):
    _, _, _, y, _ = place()
    dq[...] = dqh[...]
    for d in range(4):
        head = lanes((y + d) % 4, 128)
        dk[:, head] = kvg[d, :, 0:128]
        dv[:, head] = kvg[d, :, 128:256]
        head = lanes((y + 4 - d) % 4, 128)
        kw[:, head] = wout[d, :, 0:128]
        vw[:, head] = wout[d, :, 128:256]


VMEM = pl.BlockSpec(memory_space=pltpu.VMEM)
SMEM = pl.BlockSpec(memory_space=pltpu.SMEM)
ANY = pl.BlockSpec(memory_space=pl.ANY)


def struct(shape, dtype):
    return jax.ShapeDtypeStruct(shape, dtype)


def shards(hidden_in, queries, key_states, value_states, grad_out, log_sums, deltas, block_order):
    DMA = pltpu.SemaphoreType.DMA
    dqh, kvg, wout = pl.pallas_call(
        fused_kernel,
        out_shape=(struct((128, 2048), BF), struct((4, 128, 256), BF), struct((4, 8, 256), F32)),
        in_specs=[SMEM] + [ANY] * 7,
        out_specs=(ANY,) * 3,
        scratch_shapes=[
            pltpu.VMEM((128, 2048), BF),
            pltpu.VMEM((2, 64, 512), BF),
            pltpu.VMEM((2, 64, 512), BF),
            pltpu.VMEM((4, 128, 512), BF),
            pltpu.VMEM((4, 128, 512), BF),
            pltpu.VMEM((32, 64, 256), BF),
            pltpu.VMEM((4, 4, 128), F32),
            pltpu.VMEM((4, 4, 128), F32),
            pltpu.VMEM((4, 2048, 128), BF),
            pltpu.VMEM((8, 256, 128), BF),
            pltpu.VMEM((8, 256, 128), BF),
            pltpu.VMEM((8, 128, 256), BF),
            pltpu.VMEM((2, 256, 128), BF),
            pltpu.VMEM((2, 256, 128), BF),
            pltpu.VMEM((2, 1, 256), F32),
            pltpu.VMEM((2, 1, 256), F32),
            pltpu.VMEM((1024, 128), F32),
            pltpu.VMEM((1024, 128), F32),
            pltpu.VMEM((32, 64, 128), F32),
            pltpu.VMEM((32, 64, 128), F32),
            pltpu.VMEM((20, 256, 128), F32),
            pltpu.VMEM((20, 256, 128), F32),
            pltpu.VMEM((2, 128, 256), F32),
            pltpu.VMEM((4, 128, 512), BF),
            pltpu.VMEM((2, 512, 256), BF),
            pltpu.VMEM((2, 512, 256), BF),
            pltpu.VMEM((512, 256), BF),
            pltpu.VMEM((512, 256), BF),
            pltpu.VMEM((512, 256), BF),
            pltpu.VMEM((4, 512, 256), F32),
            pltpu.VMEM((2, 512, 256), BF),
            pltpu.VMEM((2, 512, 256), BF),
            pltpu.VMEM((512, 256), BF),
            pltpu.VMEM((512, 256), BF),
            pltpu.VMEM((16, 32, 256), BF),
            pltpu.VMEM((16, 32, 256), BF),
            pltpu.VMEM((4, 8, 256), F32),
            DMA((10, 4)),
            DMA((10, 4)),
            DMA((3, 2, 2)),
            DMA((3, 2, 2)),
            DMA((16,)),
            DMA((16,)),
            DMA((9,)),
        ],
        name="fused",
        compiler_params=pltpu.CompilerParams(collective_id=0, has_side_effects=True),
    )(
        block_order,
        queries[0],
        grad_out[0],
        key_states.reshape(2, 64, 512),
        value_states.reshape(2, 64, 512),
        log_sums.reshape(4, 4, 128),
        deltas.reshape(4, 4, 128),
        hidden_in[0],
    )
    dq, dk, dv, kw, vw = pl.pallas_call(
        finish_kernel,
        out_shape=(
            struct((128, 2048), BF),
            struct((128, 512), BF),
            struct((128, 512), BF),
            struct((8, 512), F32),
            struct((8, 512), F32),
        ),
        in_specs=[VMEM] * 3,
        out_specs=(VMEM,) * 5,
        name="finish",
    )(dqh, kvg, wout)
    return (dq[None], dk[None], dv[None], kw, vw)


def solution(mesh):
    tokens, rows = P("batch", "seq", None), P("batch", None, "seq")
    return jax.shard_map(
        shards,
        mesh=mesh,
        in_specs=(tokens, tokens, tokens, tokens, tokens, rows, rows, P()),
        out_specs=(tokens, tokens, tokens, P(("batch", "seq"), None), P(("batch", "seq"), None)),
        check_vma=False,
    )
```

```python
import math

import jax
import jax.numpy as jnp
from jax import lax
from jax.experimental import pallas as pl
from jax.experimental.pallas import tpu as pltpu
from jax.sharding import PartitionSpec as P

MESH = pl.DeviceIdType.MESH
DH = 128
SCALE = 1.0 / math.sqrt(DH)
LOG2E = math.log2(math.e)
BF = jnp.bfloat16
F32 = jnp.float32
NT = (((1,), (1,)), ((), ()))


def place():
    b, s = lax.axis_index("batch"), lax.axis_index("seq")
    return b, s, s // 8, (s // 2) % 4, s % 2


def seq_of(xh, y, c):
    return xh * 8 + y * 2 + c


def remote_copy(src, dst, send, recv, dev):
    return pltpu.make_async_remote_copy(
        src_ref=src, dst_ref=dst, send_sem=send, recv_sem=recv, device_id=dev, device_id_type=MESH
    )


def remote(*args):
    copy = remote_copy(*args)
    copy.start()
    return copy


def lanes(index, width):
    return pl.ds(pl.multiple_of(index * width, width), width)


def fused_kernel(
    order, q, do, k_in, v_in, lse, dl, hid_in, dqh, kvg, wout,
    hid, k, v, qx, dox, kvx, lx, dx, ht, ks, vs, kt, qs, dos, lsv, dlv, dka, dva, dkw, dvw, ek, ev, dqt, dqx,
    sa, ra, sx, rx, gg, acc, sb, rb, sy, ry, sf, rf, wsum,
    ssem, rsem, xsem, ysem, fsend, frecv, lsem,
):
    b, s, xh, y, c = place()
    along = [None] + [(b, seq_of(xh, (y + d) % 4, c)) for d in (1, 2, 3)]
    partner, across = (b, seq_of(xh, y, 1 - c)), (b, seq_of(1 - xh, y, c))

    keys_in = pltpu.make_async_copy(k_in, k, lsem.at[7])
    values_in = pltpu.make_async_copy(v_in, v, lsem.at[8])
    keys_in.start()
    values_in.start()
    own = [
        pltpu.make_async_copy(k_in.at[:, :, lanes(y, 128)], kvx.at[pl.ds(0, 2), :, pl.ds(0, 128)], lsem.at[0]),
        pltpu.make_async_copy(v_in.at[:, :, lanes(y, 128)], kvx.at[pl.ds(0, 2), :, pl.ds(128, 128)], lsem.at[1]),
        pltpu.make_async_copy(q.at[:, lanes(y, 512)], qx.at[0], lsem.at[2]),
        pltpu.make_async_copy(do.at[:, lanes(y, 512)], dox.at[0], lsem.at[3]),
        pltpu.make_async_copy(lse.at[y], lx.at[0], lsem.at[4]),
        pltpu.make_async_copy(dl.at[y], dx.at[0], lsem.at[5]),
    ]
    load = pltpu.make_async_copy(hid_in, hid, lsem.at[6])
    for copy in own:
        copy.start()
    load.start()

    barrier = pltpu.get_barrier_semaphore()
    for dev in (*along[1:], partner, across):
        pl.semaphore_signal(barrier, inc=1, device_id=dev, device_id_type=MESH)

    @pl.loop(1, 16)
    def _(t):
        pl.semaphore_signal(barrier, inc=1, device_id=((b + t) % 16, s), device_id_type=MESH)

    pl.semaphore_wait(barrier, 20)

    keys_in.wait()
    values_in.wait()
    kv = [[], []]
    for part, (source, half) in enumerate(((k, pl.ds(0, 128)), (v, pl.ds(128, 128)))):
        for d in (2, 1, 3):
            from_, to = source.at[:, :, lanes((y + d) % 4, 128)], kvx.at[pl.ds(2 * d, 2), :, half]
            kv[part].append(remote(from_, to, ssem.at[part, d], rsem.at[part, d], along[d]))
    rows_in = {}
    for d in (1, 3, 2):
        t = (y + d) % 4
        rows_in[d] = [
            remote(lse.at[t], lx.at[d], ssem.at[2, d], rsem.at[2, d], along[d]),
            remote(dl.at[t], dx.at[d], ssem.at[3, d], rsem.at[3, d], along[d]),
            remote(q.at[:, lanes(t, 512)], qx.at[d], ssem.at[4, d], rsem.at[4, d], along[d]),
            remote(do.at[:, lanes(t, 512)], dox.at[d], ssem.at[5, d], rsem.at[5, d], along[d]),
        ]

    load.wait()
    row = lax.broadcasted_iota(jnp.int32, (128, 128), 0)
    col = lax.broadcasted_iota(jnp.int32, (128, 128), 1)
    wanted = (row // 64) * 64 + ((row // 8) % 4) * 16 + ((row // 32) % 2) * 8 + row % 8
    pick = jnp.where(col == wanted, 1.0, 0.0).astype(BF)
    for i in range(16):
        turned = lax.dot_general(pick, hid[:, i * 128 : i * 128 + 128], NT, preferred_element_type=F32).astype(BF)
        for p in range(4):
            ht[0, p * 512 + i * 32 : p * 512 + i * 32 + 32, :] = turned[p * 32 : p * 32 + 32, :]
    feats = {}
    for d in (1, 3):
        feats[d] = remote(ht.at[0], ht.at[d], ssem.at[6, d], rsem.at[6, d], along[d])

    for copy in own:
        copy.wait()
    far, side = [], []
    for part in range(2):
        for copy in kv[part]:
            copy.wait_recv()
        half = pl.ds(part * 128, 128)
        mine, theirs = kvx.at[pl.ds(0, 8), :, half], kvx.at[pl.ds(16, 8), :, half]
        far.append(remote(mine, theirs, ssem.at[part, 0], rsem.at[part, 0], across))
        theirs = kvx.at[pl.ds(8, 8), :, half]
        side.append(remote(mine, theirs, ssem.at[2 + part, 0], rsem.at[2 + part, 0], partner))
    slot_of = [None] * 32
    firsts = [order[2 * i] for i in range(16)]
    for n in range(16):
        code = jnp.int32(0)
        for i in range(16):
            code = jnp.where(firsts[i] == n, 2 * i, jnp.where(firsts[i] == 31 - n, 2 * i + 1, code))
        pair, flip = code // 2, code % 2
        index = (((pair // 8) ^ xh) * 2 + ((pair % 2) ^ c)) * 8 + ((y + 4 - (pair // 2) % 4) % 4) * 2
        slot_of[n], slot_of[31 - n] = index + flip, index + 1 - flip
    gap = (
        lax.broadcasted_iota(jnp.int32, (256, 256), 0)
        - lax.broadcasted_iota(jnp.int32, (256, 256), 1) % 64
    )
    dka[0:1024, :] = jnp.zeros((1024, 128), F32)
    dva[0:1024, :] = jnp.zeros((1024, 128), F32)
    last = []
    for part in range(2):
        far[part].wait_recv()
        half = pl.ds(part * 128, 128)
        mine, theirs = kvx.at[pl.ds(16, 8), :, half], kvx.at[pl.ds(24, 8), :, half]
        last.append(remote(mine, theirs, ssem.at[4 + part, 0], rsem.at[4 + part, 0], partner))
    for copy in (*side, *last):
        copy.wait_recv()
    for n in range(32):
        both = kvx[slot_of[n]]
        ks[n // 4, n % 4 * 64 : n % 4 * 64 + 64, :] = both[:, 0:128]
        vs[n // 4, n % 4 * 64 : n % 4 * 64 + 64, :] = both[:, 128:256]
    for n in range(8):
        kt[n] = ks[n].T

    def first_of(d):
        return order[seq_of(xh, (y + 4 - d) % 4, c) * 2]

    def low_of(d):
        first = first_of(d)
        return jnp.minimum(first, 31 - first)

    def products(h, n, block):
        scores = lax.dot_general(ks[n], qs[h], NT, preferred_element_type=F32)
        dprobs = lax.dot_general(vs[n], dos[h], NT, preferred_element_type=F32)
        return h, n, block, scores, dprobs

    def parts(h, n, block, scores, dprobs):
        probs = jnp.exp2(scores * (SCALE * LOG2E) - lsv[h])
        if block is not None:
            probs = jnp.where(gap <= block * 64 - n * 256, probs, 0.0)
        dscores = (probs * (dprobs - dlv[h]) * SCALE).astype(BF)
        return (
            jnp.dot(dscores, qs[h], preferred_element_type=F32),
            jnp.dot(probs.astype(BF), dos[h], preferred_element_type=F32),
            jnp.dot(kt[n], dscores, preferred_element_type=F32),
        )

    def home_copy(d):
        dev = (b, seq_of(xh, (y + 4 - d) % 4, c))
        return remote_copy(dqx.at[d], dqh.at[:, lanes(y, 512)], ssem.at[7, d], rsem.at[7, d], dev)

    lane = lax.broadcasted_iota(jnp.int32, (1, 128), 1) < 64

    @pl.loop(0, 4)
    def _(turn):
        d = jnp.where(turn == 2, 3, jnp.where(turn == 3, 2, turn))

        @pl.when(turn > 0)
        def _():
            dev = (b, seq_of(xh, (y + 4 - d) % 4, c))
            remote_copy(lse.at[0], lx.at[d], ssem.at[2, d], rsem.at[2, d], dev).wait_recv()
            remote_copy(dl.at[0], dx.at[d], ssem.at[3, d], rsem.at[3, d], dev).wait_recv()
            remote_copy(q.at[:, pl.ds(0, 512)], qx.at[d], ssem.at[4, d], rsem.at[4, d], dev).wait_recv()
            remote_copy(do.at[:, pl.ds(0, 512)], dox.at[d], ssem.at[5, d], rsem.at[5, d], dev).wait_recv()

        flip = first_of(d) >= 16
        low = low_of(d)
        quad = low // 4
        for source, target in ((qx, qs), (dox, dos)):
            for h in range(4):
                zero = source[d, 0:64, h * 128 : h * 128 + 128]
                one = source[d, 64:128, h * 128 : h * 128 + 128]
                target[0, h * 64 : h * 64 + 64, :] = jnp.where(flip, one, zero)
                target[1, h * 64 : h * 64 + 64, :] = jnp.where(flip, zero, one)
        for source, target, factor in ((lx, lsv, LOG2E), (dx, dlv, None)):
            plain = source[d]
            rolled = pltpu.roll(plain, 64, axis=1)
            pairs = []
            for left, right in ((plain, rolled), (rolled, plain)):
                line = jnp.concatenate(
                    [jnp.where(lane, left[h : h + 1, :], right[h + 1 : h + 2, :]) for h in (0, 2)], axis=1
                )
                pairs.append(line if factor is None else line * factor)
            target[0] = jnp.where(flip, pairs[1], pairs[0])
            target[1] = jnp.where(flip, pairs[0], pairs[1])
        dqt[...] = jnp.zeros_like(dqt)
        lows = [j <= quad for j in range(4)]
        todo = [(1, n, None) for n in range(4)]
        todo += [
            (jnp.where(lows[j], 0, 1), jnp.where(lows[j], j, 7 - j), jnp.where(lows[j], low, 31 - low))
            for j in range(4)
        ]
        todo.append((1, 7 - quad, 31 - low))
        ahead = products(*todo[0])
        for i in range(9):
            now = ahead
            if i < 8:
                ahead = products(*todo[i + 1])
            dk, dv, dq = parts(*now)
            if i < 4:
                dka[i * 256 : i * 256 + 256, :] += dk
                dva[i * 256 : i * 256 + 256, :] += dv
                dqt[1] += dq
                continue
            ek[d * 5 + i - 4] = dk
            ev[d * 5 + i - 4] = dv
            if i < 8:
                dqt[0] += jnp.where(lows[i - 4], dq, 0.0)
                dqt[1] += jnp.where(lows[i - 4], 0.0, dq)
            else:
                dqt[1] += dq
        low_q, high_q = dqt[0].T, dqt[1].T
        for h in range(4):
            lo, hi = low_q[h * 64 : h * 64 + 64, :].astype(BF), high_q[h * 64 : h * 64 + 64, :].astype(BF)
            dqx[d, 0:64, h * 128 : h * 128 + 128] = jnp.where(flip, hi, lo)
            dqx[d, 64:128, h * 128 : h * 128 + 128] = jnp.where(flip, lo, hi)

    own_q = pltpu.make_async_copy(dqx.at[0], dqh.at[:, lanes(y, 512)], lsem.at[0])
    own_q.start()
    quads = [low_of(d) // 4 for d in range(4)]

    @pl.loop(0, 4)
    def _(part):
        for n in range(8):
            at = pl.ds(pl.multiple_of(n * 256 + part * 64, 64), 64)
            sub = pl.ds(pl.multiple_of(part * 64, 64), 64)
            for store, extra, whole in ((dka, ek, dkw), (dva, ev, dvw)):
                total = store[at, :] if n < 4 else jnp.zeros((64, 128), F32)
                for d in range(4):
                    if n < 4:
                        total += jnp.where(n <= quads[d], extra[d * 5 + n, sub, :], 0.0)
                    else:
                        total += jnp.where(7 - n > quads[d], extra[d * 5 + 7 - n, sub, :], 0.0)
                        total += jnp.where(7 - n == quads[d], extra[d * 5 + 4, sub, :], 0.0)
                whole[n * 4 + part] = total

    def summed(part, put, between, after, send, recv, send_far, recv_far, sems):
        blocks = [slice(i * 64, i * 64 + 64) for i in range(8)]
        chunks = [(n, pl.ds(n * 256, 256), range(n * 4, n * 4 + 4)) for n in range(2)]
        one, two, far = [], [], []
        for n, rows, members in chunks:
            for i in members:
                send[1, blocks[i], :] = part(3, i).astype(BF)
            one.append(remote(send.at[1, rows], recv.at[1, rows], sems.at[0, 0, n], sems.at[0, 1, n], partner))
        for n, rows, members in chunks:
            one[n].wait_recv()
            for i in members:
                send_far[blocks[i], :] = (part(2, i) + recv[1, blocks[i], :].astype(F32)).astype(BF)
            far.append(remote(send_far.at[rows], recv_far.at[rows], sems.at[2, 0, n], sems.at[2, 1, n], across))
        between()
        for n, rows, members in chunks:
            for i in members:
                send[0, blocks[i], :] = part(1, i).astype(BF)
            two.append(remote(send.at[0, rows], recv.at[0, rows], sems.at[1, 0, n], sems.at[1, 1, n], partner))
        for n, rows, members in chunks:
            two[n].wait_recv()
            far[n].wait_recv()
            for i in members:
                put(i, part(0, i) + recv[0, blocks[i], :].astype(F32) + recv_far[blocks[i], :].astype(F32))
            after(n)
        return one + two + far

    def grads_part(m, i):
        block = order[seq_of(xh ^ (m >> 1), (y + 4 - i // 2) % 4, c ^ (m & 1)) * 2 + i % 2]
        return jnp.concatenate([dkw[block], dvw[block]], axis=1)

    def put_grads(i, value):
        gg[i * 64 : i * 64 + 64, :] = value.astype(BF)

    relays = []

    def relay():
        for d in (1, 3):
            feats[d].wait_recv()
        for late in range(2):
            for d in (1, 3):
                at = ((1 - xh) if late == 0 else xh) * 2 + d // 2
                rows = pl.ds(pl.multiple_of(at * 512, 512), 512)
                sems = (ssem.at[9 + 2 * late, d], rsem.at[9 + 2 * late, d])
                relays.append(remote(ht.at[d, rows], ht.at[2, rows], *sems, along[d]))

    sent = summed(grads_part, put_grads, relay, lambda n: None, sa, ra, sx, rx, xsem)
    back = []
    for d in (1, 2, 3):
        back.append(remote(gg.at[pl.ds(d * 128, 128)], kvg.at[d], ssem.at[8, d], rsem.at[8, d], along[4 - d]))
    own_g = pltpu.make_async_copy(gg.at[pl.ds(0, 128)], kvg.at[0], lsem.at[1])
    own_g.start()

    def outer(m):
        at = (xh ^ (m >> 1)) * 2 + (c ^ (m & 1))
        rows = pl.ds(pl.multiple_of(at * 512, 512), 512)
        features = jnp.concatenate([ht[d, rows, :] for d in range(4)], axis=1)
        acc[m] = jnp.dot(features, gg[...], preferred_element_type=F32)

    for copy in relays[:2]:
        copy.wait_recv()
    outer(3)
    outer(2)

    def rest():
        for copy in relays[2:]:
            copy.wait_recv()
        outer(1)
        outer(0)
        for d in (1, 3, 2):
            home_copy(d).start()

    def put_rows(i, value):
        sf[2 * i] = value[0:32, :].astype(BF)
        sf[2 * i + 1] = value[32:64, :].astype(BF)

    def batch_copy(t):
        to = (b + t) % 16
        return remote_copy(sf.at[to], rf.at[t], fsend.at[t], frecv.at[t], (to, s))

    def spread(n):
        @pl.loop(n * 8, n * 8 + 8)
        def _(to):
            @pl.when(to != b)
            def _():
                batch_copy((to + 16 - b) % 16).start()

    sent += summed(lambda m, i: acc[m, i * 64 : i * 64 + 64, :], put_rows, rest, spread, sb, rb, sy, ry, ysem)
    rf[0] = sf[b]

    @pl.loop(1, 16)
    def _(t):
        batch_copy(t).wait_recv()

    total = jnp.sum(rf[...].astype(F32), axis=0)
    for t in range(4):
        wsum[t] = total[t * 8 : t * 8 + 8, :]
    tail = [remote(wsum.at[(y + d) % 4], wout.at[d], ssem.at[10, d], rsem.at[10, d], along[d]) for d in (1, 2, 3)]
    own_w = pltpu.make_async_copy(wsum.at[y], wout.at[0], lsem.at[2])
    own_w.start()

    @pl.loop(1, 16)
    def _(t):
        batch_copy(t).wait_send()

    for copy in (own_q, own_g, own_w):
        copy.wait()
    for d in (1, 2, 3):
        home_copy(d).wait()
        for copy in rows_in[d]:
            copy.wait_send()
    for copy in (feats[1], feats[3], *relays, *kv[0], *kv[1], *far, *side, *last, *sent):
        copy.wait_send()
    for copy in (*back, *tail):
        copy.wait()


def finish_kernel(dqh, kvg, wout, dq, dk, dv, kw, vw):
    _, _, _, y, _ = place()
    dq[...] = dqh[...]
    for d in range(4):
        head = lanes((y + d) % 4, 128)
        dk[:, head] = kvg[d, :, 0:128]
        dv[:, head] = kvg[d, :, 128:256]
        head = lanes((y + 4 - d) % 4, 128)
        kw[:, head] = wout[d, :, 0:128]
        vw[:, head] = wout[d, :, 128:256]


VMEM = pl.BlockSpec(memory_space=pltpu.VMEM)
SMEM = pl.BlockSpec(memory_space=pltpu.SMEM)
ANY = pl.BlockSpec(memory_space=pl.ANY)


def struct(shape, dtype):
    return jax.ShapeDtypeStruct(shape, dtype)


def shards(hidden_in, queries, key_states, value_states, grad_out, log_sums, deltas, block_order):
    DMA = pltpu.SemaphoreType.DMA
    dqh, kvg, wout = pl.pallas_call(
        fused_kernel,
        out_shape=(struct((128, 2048), BF), struct((4, 128, 256), BF), struct((4, 8, 256), F32)),
        in_specs=[SMEM] + [ANY] * 7,
        out_specs=(ANY,) * 3,
        scratch_shapes=[
            pltpu.VMEM((128, 2048), BF),
            pltpu.VMEM((2, 64, 512), BF),
            pltpu.VMEM((2, 64, 512), BF),
            pltpu.VMEM((4, 128, 512), BF),
            pltpu.VMEM((4, 128, 512), BF),
            pltpu.VMEM((32, 64, 256), BF),
            pltpu.VMEM((4, 4, 128), F32),
            pltpu.VMEM((4, 4, 128), F32),
            pltpu.VMEM((4, 2048, 128), BF),
            pltpu.VMEM((8, 256, 128), BF),
            pltpu.VMEM((8, 256, 128), BF),
            pltpu.VMEM((8, 128, 256), BF),
            pltpu.VMEM((2, 256, 128), BF),
            pltpu.VMEM((2, 256, 128), BF),
            pltpu.VMEM((2, 1, 256), F32),
            pltpu.VMEM((2, 1, 256), F32),
            pltpu.VMEM((1024, 128), F32),
            pltpu.VMEM((1024, 128), F32),
            pltpu.VMEM((32, 64, 128), F32),
            pltpu.VMEM((32, 64, 128), F32),
            pltpu.VMEM((20, 256, 128), F32),
            pltpu.VMEM((20, 256, 128), F32),
            pltpu.VMEM((2, 128, 256), F32),
            pltpu.VMEM((4, 128, 512), BF),
            pltpu.VMEM((2, 512, 256), BF),
            pltpu.VMEM((2, 512, 256), BF),
            pltpu.VMEM((512, 256), BF),
            pltpu.VMEM((512, 256), BF),
            pltpu.VMEM((512, 256), BF),
            pltpu.VMEM((4, 512, 256), F32),
            pltpu.VMEM((2, 512, 256), BF),
            pltpu.VMEM((2, 512, 256), BF),
            pltpu.VMEM((512, 256), BF),
            pltpu.VMEM((512, 256), BF),
            pltpu.VMEM((16, 32, 256), BF),
            pltpu.VMEM((16, 32, 256), BF),
            pltpu.VMEM((4, 8, 256), F32),
            DMA((12, 4)),
            DMA((12, 4)),
            DMA((3, 2, 2)),
            DMA((3, 2, 2)),
            DMA((16,)),
            DMA((16,)),
            DMA((9,)),
        ],
        name="fused",
        compiler_params=pltpu.CompilerParams(collective_id=0, has_side_effects=True),
    )(
        block_order,
        queries[0],
        grad_out[0],
        key_states.reshape(2, 64, 512),
        value_states.reshape(2, 64, 512),
        log_sums.reshape(4, 4, 128),
        deltas.reshape(4, 4, 128),
        hidden_in[0],
    )
    dq, dk, dv, kw, vw = pl.pallas_call(
        finish_kernel,
        out_shape=(
            struct((128, 2048), BF),
            struct((128, 512), BF),
            struct((128, 512), BF),
            struct((8, 512), F32),
            struct((8, 512), F32),
        ),
        in_specs=[VMEM] * 3,
        out_specs=(VMEM,) * 5,
        name="finish",
    )(dqh, kvg, wout)
    return (dq[None], dk[None], dv[None], kw, vw)


def solution(mesh):
    tokens, rows = P("batch", "seq", None), P("batch", None, "seq")
    return jax.shard_map(
        shards,
        mesh=mesh,
        in_specs=(tokens, tokens, tokens, tokens, tokens, rows, rows, P()),
        out_specs=(tokens, tokens, tokens, P(("batch", "seq"), None), P(("batch", "seq"), None)),
        check_vma=False,
    )
```

```python
import math

import jax
import jax.numpy as jnp
from jax import lax
from jax.experimental import pallas as pl
from jax.experimental.pallas import tpu as pltpu
from jax.sharding import PartitionSpec as P

MESH = pl.DeviceIdType.MESH
DH = 128
SCALE = 1.0 / math.sqrt(DH)
LOG2E = math.log2(math.e)
BF = jnp.bfloat16
F32 = jnp.float32
NT = (((1,), (1,)), ((), ()))


def place():
    b, s = lax.axis_index("batch"), lax.axis_index("seq")
    return b, s, s // 8, (s // 2) % 4, s % 2


def seq_of(xh, y, c):
    return xh * 8 + y * 2 + c


def remote_copy(src, dst, send, recv, dev):
    return pltpu.make_async_remote_copy(
        src_ref=src, dst_ref=dst, send_sem=send, recv_sem=recv, device_id=dev, device_id_type=MESH
    )


def remote(*args):
    copy = remote_copy(*args)
    copy.start()
    return copy


def lanes(index, width):
    return pl.ds(pl.multiple_of(index * width, width), width)


def fused_kernel(
    order, q, do, k_in, v_in, lse, dl, hid_in, dqh, kvg, wout,
    hid, k, v, qx, dox, kvx, lx, dx, ht, ks, vs, kt, qs, dos, lsv, dlv, dka, dva, dkw, dvw, ek, ev, dqt, dqx,
    sa, ra, sx, rx, gg, acc, sb, rb, sy, ry, sf, rf, wsum,
    ssem, rsem, xsem, ysem, fsend, frecv, lsem,
):
    b, s, xh, y, c = place()
    along = [None] + [(b, seq_of(xh, (y + d) % 4, c)) for d in (1, 2, 3)]
    partner, across = (b, seq_of(xh, y, 1 - c)), (b, seq_of(1 - xh, y, c))

    keys_in = pltpu.make_async_copy(k_in, k, lsem.at[7])
    values_in = pltpu.make_async_copy(v_in, v, lsem.at[8])
    keys_in.start()
    values_in.start()
    own = [
        pltpu.make_async_copy(k_in.at[:, :, lanes(y, 128)], kvx.at[pl.ds(0, 2), :, pl.ds(0, 128)], lsem.at[0]),
        pltpu.make_async_copy(v_in.at[:, :, lanes(y, 128)], kvx.at[pl.ds(0, 2), :, pl.ds(128, 128)], lsem.at[1]),
        pltpu.make_async_copy(q.at[:, lanes(y, 512)], qx.at[0], lsem.at[2]),
        pltpu.make_async_copy(do.at[:, lanes(y, 512)], dox.at[0], lsem.at[3]),
        pltpu.make_async_copy(lse.at[y], lx.at[0], lsem.at[4]),
        pltpu.make_async_copy(dl.at[y], dx.at[0], lsem.at[5]),
    ]
    load = pltpu.make_async_copy(hid_in, hid, lsem.at[6])
    for copy in own:
        copy.start()
    load.start()

    barrier = pltpu.get_barrier_semaphore()
    for dev in (*along[1:], partner, across):
        pl.semaphore_signal(barrier, inc=1, device_id=dev, device_id_type=MESH)

    @pl.loop(1, 16)
    def _(t):
        pl.semaphore_signal(barrier, inc=1, device_id=((b + t) % 16, s), device_id_type=MESH)

    pl.semaphore_wait(barrier, 20)

    keys_in.wait()
    values_in.wait()
    kv = [[], []]
    for part, (source, half) in enumerate(((k, pl.ds(0, 128)), (v, pl.ds(128, 128)))):
        for d in (2, 1, 3):
            from_, to = source.at[:, :, lanes((y + d) % 4, 128)], kvx.at[pl.ds(2 * d, 2), :, half]
            kv[part].append(remote(from_, to, ssem.at[part, d], rsem.at[part, d], along[d]))
    rows_in = {}
    for d in (1, 3, 2):
        t = (y + d) % 4
        rows_in[d] = [
            remote(lse.at[t], lx.at[d], ssem.at[2, d], rsem.at[2, d], along[d]),
            remote(dl.at[t], dx.at[d], ssem.at[3, d], rsem.at[3, d], along[d]),
            remote(q.at[:, lanes(t, 512)], qx.at[d], ssem.at[4, d], rsem.at[4, d], along[d]),
            remote(do.at[:, lanes(t, 512)], dox.at[d], ssem.at[5, d], rsem.at[5, d], along[d]),
        ]

    load.wait()
    row = lax.broadcasted_iota(jnp.int32, (128, 128), 0)
    col = lax.broadcasted_iota(jnp.int32, (128, 128), 1)
    wanted = (row // 64) * 64 + ((row // 8) % 4) * 16 + ((row // 32) % 2) * 8 + row % 8
    pick = jnp.where(col == wanted, 1.0, 0.0).astype(BF)
    for i in range(16):
        turned = lax.dot_general(pick, hid[:, i * 128 : i * 128 + 128], NT, preferred_element_type=F32).astype(BF)
        for p in range(4):
            ht[0, p * 512 + i * 32 : p * 512 + i * 32 + 32, :] = turned[p * 32 : p * 32 + 32, :]
    feats = {}
    for late in range(2):
        rows = pl.ds(pl.multiple_of((xh if late else 1 - xh) * 1024, 1024), 1024)
        for d in (1, 3):
            sems = (ssem.at[6 + 6 * late, d], rsem.at[6 + 6 * late, d])
            feats[d, late] = remote(ht.at[0, rows], ht.at[d, rows], *sems, along[d])

    for copy in own:
        copy.wait()
    far, side = [], []
    for part in range(2):
        for copy in kv[part]:
            copy.wait_recv()
        half = pl.ds(part * 128, 128)
        mine, theirs = kvx.at[pl.ds(0, 8), :, half], kvx.at[pl.ds(16, 8), :, half]
        far.append(remote(mine, theirs, ssem.at[part, 0], rsem.at[part, 0], across))
        theirs = kvx.at[pl.ds(8, 8), :, half]
        side.append(remote(mine, theirs, ssem.at[2 + part, 0], rsem.at[2 + part, 0], partner))
    slot_of = [None] * 32
    firsts = [order[2 * i] for i in range(16)]
    for n in range(16):
        code = jnp.int32(0)
        for i in range(16):
            code = jnp.where(firsts[i] == n, 2 * i, jnp.where(firsts[i] == 31 - n, 2 * i + 1, code))
        pair, flip = code // 2, code % 2
        index = (((pair // 8) ^ xh) * 2 + ((pair % 2) ^ c)) * 8 + ((y + 4 - (pair // 2) % 4) % 4) * 2
        slot_of[n], slot_of[31 - n] = index + flip, index + 1 - flip
    gap = (
        lax.broadcasted_iota(jnp.int32, (256, 256), 0)
        - lax.broadcasted_iota(jnp.int32, (256, 256), 1) % 64
    )
    dka[0:1024, :] = jnp.zeros((1024, 128), F32)
    dva[0:1024, :] = jnp.zeros((1024, 128), F32)
    last = []
    for part in range(2):
        far[part].wait_recv()
        half = pl.ds(part * 128, 128)
        mine, theirs = kvx.at[pl.ds(16, 8), :, half], kvx.at[pl.ds(24, 8), :, half]
        last.append(remote(mine, theirs, ssem.at[4 + part, 0], rsem.at[4 + part, 0], partner))
    for copy in (*side, *last):
        copy.wait_recv()
    for n in range(32):
        both = kvx[slot_of[n]]
        ks[n // 4, n % 4 * 64 : n % 4 * 64 + 64, :] = both[:, 0:128]
        vs[n // 4, n % 4 * 64 : n % 4 * 64 + 64, :] = both[:, 128:256]
    for n in range(8):
        kt[n] = ks[n].T

    def first_of(d):
        return order[seq_of(xh, (y + 4 - d) % 4, c) * 2]

    def low_of(d):
        first = first_of(d)
        return jnp.minimum(first, 31 - first)

    def products(h, n, block):
        scores = lax.dot_general(ks[n], qs[h], NT, preferred_element_type=F32)
        dprobs = lax.dot_general(vs[n], dos[h], NT, preferred_element_type=F32)
        return h, n, block, scores, dprobs

    def parts(h, n, block, scores, dprobs):
        probs = jnp.exp2(scores * (SCALE * LOG2E) - lsv[h])
        if block is not None:
            probs = jnp.where(gap <= block * 64 - n * 256, probs, 0.0)
        dscores = (probs * (dprobs - dlv[h]) * SCALE).astype(BF)
        return (
            jnp.dot(dscores, qs[h], preferred_element_type=F32),
            jnp.dot(probs.astype(BF), dos[h], preferred_element_type=F32),
            jnp.dot(kt[n], dscores, preferred_element_type=F32),
        )

    def home_copy(d):
        dev = (b, seq_of(xh, (y + 4 - d) % 4, c))
        return remote_copy(dqx.at[d], dqh.at[:, lanes(y, 512)], ssem.at[7, d], rsem.at[7, d], dev)

    lane = lax.broadcasted_iota(jnp.int32, (1, 128), 1) < 64

    @pl.loop(0, 4)
    def _(turn):
        d = jnp.where(turn == 2, 3, jnp.where(turn == 3, 2, turn))

        @pl.when(turn > 0)
        def _():
            dev = (b, seq_of(xh, (y + 4 - d) % 4, c))
            remote_copy(lse.at[0], lx.at[d], ssem.at[2, d], rsem.at[2, d], dev).wait_recv()
            remote_copy(dl.at[0], dx.at[d], ssem.at[3, d], rsem.at[3, d], dev).wait_recv()
            remote_copy(q.at[:, pl.ds(0, 512)], qx.at[d], ssem.at[4, d], rsem.at[4, d], dev).wait_recv()
            remote_copy(do.at[:, pl.ds(0, 512)], dox.at[d], ssem.at[5, d], rsem.at[5, d], dev).wait_recv()

        flip = first_of(d) >= 16
        low = low_of(d)
        quad = low // 4
        for source, target in ((qx, qs), (dox, dos)):
            for h in range(4):
                zero = source[d, 0:64, h * 128 : h * 128 + 128]
                one = source[d, 64:128, h * 128 : h * 128 + 128]
                target[0, h * 64 : h * 64 + 64, :] = jnp.where(flip, one, zero)
                target[1, h * 64 : h * 64 + 64, :] = jnp.where(flip, zero, one)
        for source, target, factor in ((lx, lsv, LOG2E), (dx, dlv, None)):
            plain = source[d]
            rolled = pltpu.roll(plain, 64, axis=1)
            pairs = []
            for left, right in ((plain, rolled), (rolled, plain)):
                line = jnp.concatenate(
                    [jnp.where(lane, left[h : h + 1, :], right[h + 1 : h + 2, :]) for h in (0, 2)], axis=1
                )
                pairs.append(line if factor is None else line * factor)
            target[0] = jnp.where(flip, pairs[1], pairs[0])
            target[1] = jnp.where(flip, pairs[0], pairs[1])
        dqt[...] = jnp.zeros_like(dqt)
        lows = [j <= quad for j in range(4)]
        todo = [(1, n, None) for n in range(4)]
        todo += [
            (jnp.where(lows[j], 0, 1), jnp.where(lows[j], j, 7 - j), jnp.where(lows[j], low, 31 - low))
            for j in range(4)
        ]
        todo.append((1, 7 - quad, 31 - low))
        ahead = products(*todo[0])
        for i in range(9):
            now = ahead
            if i < 8:
                ahead = products(*todo[i + 1])
            dk, dv, dq = parts(*now)
            if i < 4:
                dka[i * 256 : i * 256 + 256, :] += dk
                dva[i * 256 : i * 256 + 256, :] += dv
                dqt[1] += dq
                continue
            ek[d * 5 + i - 4] = dk
            ev[d * 5 + i - 4] = dv
            if i < 8:
                dqt[0] += jnp.where(lows[i - 4], dq, 0.0)
                dqt[1] += jnp.where(lows[i - 4], 0.0, dq)
            else:
                dqt[1] += dq
        low_q, high_q = dqt[0].T, dqt[1].T
        for h in range(4):
            lo, hi = low_q[h * 64 : h * 64 + 64, :].astype(BF), high_q[h * 64 : h * 64 + 64, :].astype(BF)
            dqx[d, 0:64, h * 128 : h * 128 + 128] = jnp.where(flip, hi, lo)
            dqx[d, 64:128, h * 128 : h * 128 + 128] = jnp.where(flip, lo, hi)

    own_q = pltpu.make_async_copy(dqx.at[0], dqh.at[:, lanes(y, 512)], lsem.at[0])
    own_q.start()
    quads = [low_of(d) // 4 for d in range(4)]

    @pl.loop(0, 4)
    def _(part):
        for n in range(8):
            at = pl.ds(pl.multiple_of(n * 256 + part * 64, 64), 64)
            sub = pl.ds(pl.multiple_of(part * 64, 64), 64)
            for store, extra, whole in ((dka, ek, dkw), (dva, ev, dvw)):
                total = store[at, :] if n < 4 else jnp.zeros((64, 128), F32)
                for d in range(4):
                    if n < 4:
                        total += jnp.where(n <= quads[d], extra[d * 5 + n, sub, :], 0.0)
                    else:
                        total += jnp.where(7 - n > quads[d], extra[d * 5 + 7 - n, sub, :], 0.0)
                        total += jnp.where(7 - n == quads[d], extra[d * 5 + 4, sub, :], 0.0)
                whole[n * 4 + part] = total

    def summed(part, put, between, behind, after, send, recv, send_far, recv_far, sems):
        blocks = [slice(i * 64, i * 64 + 64) for i in range(8)]
        chunks = [(n, pl.ds(n * 256, 256), range(n * 4, n * 4 + 4)) for n in range(2)]
        one, two, far = [], [], []
        for n, rows, members in chunks:
            for i in members:
                send[1, blocks[i], :] = part(3, i).astype(BF)
            one.append(remote(send.at[1, rows], recv.at[1, rows], sems.at[0, 0, n], sems.at[0, 1, n], partner))
        for n, rows, members in chunks:
            one[n].wait_recv()
            for i in members:
                send_far[blocks[i], :] = (part(2, i) + recv[1, blocks[i], :].astype(F32)).astype(BF)
            far.append(remote(send_far.at[rows], recv_far.at[rows], sems.at[2, 0, n], sems.at[2, 1, n], across))
        between()
        for n, rows, members in chunks:
            for i in members:
                send[0, blocks[i], :] = part(1, i).astype(BF)
            two.append(remote(send.at[0, rows], recv.at[0, rows], sems.at[1, 0, n], sems.at[1, 1, n], partner))
        behind()
        for n, rows, members in chunks:
            two[n].wait_recv()
            far[n].wait_recv()
            for i in members:
                put(i, part(0, i) + recv[0, blocks[i], :].astype(F32) + recv_far[blocks[i], :].astype(F32))
            after(n)
        return one + two + far

    def grads_part(m, i):
        block = order[seq_of(xh ^ (m >> 1), (y + 4 - i // 2) % 4, c ^ (m & 1)) * 2 + i % 2]
        return jnp.concatenate([dkw[block], dvw[block]], axis=1)

    def put_grads(i, value):
        gg[i * 64 : i * 64 + 64, :] = value.astype(BF)

    relays = []

    def relay(late):
        for d in (1, 3):
            feats[d, late].wait_recv()
            rows = pl.ds(pl.multiple_of(((xh if late else 1 - xh) * 2 + d // 2) * 512, 512), 512)
            sems = (ssem.at[9 + 2 * late, d], rsem.at[9 + 2 * late, d])
            relays.append(remote(ht.at[d, rows], ht.at[2, rows], *sems, along[d]))

    sent = summed(grads_part, put_grads, lambda: relay(0), lambda: relay(1), lambda n: None, sa, ra, sx, rx, xsem)
    back = []
    own_g = pltpu.make_async_copy(gg.at[pl.ds(0, 128)], kvg.at[0], lsem.at[1])
    own_g.start()

    def outer(m):
        at = (xh ^ (m >> 1)) * 2 + (c ^ (m & 1))
        rows = pl.ds(pl.multiple_of(at * 512, 512), 512)
        features = jnp.concatenate([ht[d, rows, :] for d in range(4)], axis=1)
        acc[m] = jnp.dot(features, gg[...], preferred_element_type=F32)

    for copy in relays[:2]:
        copy.wait_recv()
    outer(3)
    outer(2)

    def rest():
        for copy in relays[2:]:
            copy.wait_recv()
        outer(1)
        outer(0)
        for d in (1, 3, 2):
            home_copy(d).start()
        for d in (1, 2, 3):
            back.append(remote(gg.at[pl.ds(d * 128, 128)], kvg.at[d], ssem.at[8, d], rsem.at[8, d], along[4 - d]))

    def put_rows(i, value):
        sf[2 * i] = value[0:32, :].astype(BF)
        sf[2 * i + 1] = value[32:64, :].astype(BF)

    def batch_copy(t):
        to = (b + t) % 16
        return remote_copy(sf.at[to], rf.at[t], fsend.at[t], frecv.at[t], (to, s))

    def spread(n):
        @pl.loop(n * 8, n * 8 + 8)
        def _(to):
            @pl.when(to != b)
            def _():
                batch_copy((to + 16 - b) % 16).start()

    sent += summed(lambda m, i: acc[m, i * 64 : i * 64 + 64, :], put_rows, rest, lambda: None, spread, sb, rb, sy, ry, ysem)
    rf[0] = sf[b]

    @pl.loop(1, 16)
    def _(t):
        batch_copy(t).wait_recv()

    total = jnp.sum(rf[...].astype(F32), axis=0)
    for t in range(4):
        wsum[t] = total[t * 8 : t * 8 + 8, :]
    tail = [remote(wsum.at[(y + d) % 4], wout.at[d], ssem.at[10, d], rsem.at[10, d], along[d]) for d in (1, 2, 3)]
    own_w = pltpu.make_async_copy(wsum.at[y], wout.at[0], lsem.at[2])
    own_w.start()

    @pl.loop(1, 16)
    def _(t):
        batch_copy(t).wait_send()

    for copy in (own_q, own_g, own_w):
        copy.wait()
    for d in (1, 2, 3):
        home_copy(d).wait()
        for copy in rows_in[d]:
            copy.wait_send()
    for copy in (*feats.values(), *relays, *kv[0], *kv[1], *far, *side, *last, *sent):
        copy.wait_send()
    for copy in (*back, *tail):
        copy.wait()


def finish_kernel(dqh, kvg, wout, dq, dk, dv, kw, vw):
    _, _, _, y, _ = place()
    dq[...] = dqh[...]
    for d in range(4):
        head = lanes((y + d) % 4, 128)
        dk[:, head] = kvg[d, :, 0:128]
        dv[:, head] = kvg[d, :, 128:256]
        head = lanes((y + 4 - d) % 4, 128)
        kw[:, head] = wout[d, :, 0:128]
        vw[:, head] = wout[d, :, 128:256]


VMEM = pl.BlockSpec(memory_space=pltpu.VMEM)
SMEM = pl.BlockSpec(memory_space=pltpu.SMEM)
ANY = pl.BlockSpec(memory_space=pl.ANY)


def struct(shape, dtype):
    return jax.ShapeDtypeStruct(shape, dtype)


def shards(hidden_in, queries, key_states, value_states, grad_out, log_sums, deltas, block_order):
    DMA = pltpu.SemaphoreType.DMA
    dqh, kvg, wout = pl.pallas_call(
        fused_kernel,
        out_shape=(struct((128, 2048), BF), struct((4, 128, 256), BF), struct((4, 8, 256), F32)),
        in_specs=[SMEM] + [ANY] * 7,
        out_specs=(ANY,) * 3,
        scratch_shapes=[
            pltpu.VMEM((128, 2048), BF),
            pltpu.VMEM((2, 64, 512), BF),
            pltpu.VMEM((2, 64, 512), BF),
            pltpu.VMEM((4, 128, 512), BF),
            pltpu.VMEM((4, 128, 512), BF),
            pltpu.VMEM((32, 64, 256), BF),
            pltpu.VMEM((4, 4, 128), F32),
            pltpu.VMEM((4, 4, 128), F32),
            pltpu.VMEM((4, 2048, 128), BF),
            pltpu.VMEM((8, 256, 128), BF),
            pltpu.VMEM((8, 256, 128), BF),
            pltpu.VMEM((8, 128, 256), BF),
            pltpu.VMEM((2, 256, 128), BF),
            pltpu.VMEM((2, 256, 128), BF),
            pltpu.VMEM((2, 1, 256), F32),
            pltpu.VMEM((2, 1, 256), F32),
            pltpu.VMEM((1024, 128), F32),
            pltpu.VMEM((1024, 128), F32),
            pltpu.VMEM((32, 64, 128), F32),
            pltpu.VMEM((32, 64, 128), F32),
            pltpu.VMEM((20, 256, 128), F32),
            pltpu.VMEM((20, 256, 128), F32),
            pltpu.VMEM((2, 128, 256), F32),
            pltpu.VMEM((4, 128, 512), BF),
            pltpu.VMEM((2, 512, 256), BF),
            pltpu.VMEM((2, 512, 256), BF),
            pltpu.VMEM((512, 256), BF),
            pltpu.VMEM((512, 256), BF),
            pltpu.VMEM((512, 256), BF),
            pltpu.VMEM((4, 512, 256), F32),
            pltpu.VMEM((2, 512, 256), BF),
            pltpu.VMEM((2, 512, 256), BF),
            pltpu.VMEM((512, 256), BF),
            pltpu.VMEM((512, 256), BF),
            pltpu.VMEM((16, 32, 256), BF),
            pltpu.VMEM((16, 32, 256), BF),
            pltpu.VMEM((4, 8, 256), F32),
            DMA((13, 4)),
            DMA((13, 4)),
            DMA((3, 2, 2)),
            DMA((3, 2, 2)),
            DMA((16,)),
            DMA((16,)),
            DMA((9,)),
        ],
        name="fused",
        compiler_params=pltpu.CompilerParams(collective_id=0, has_side_effects=True),
    )(
        block_order,
        queries[0],
        grad_out[0],
        key_states.reshape(2, 64, 512),
        value_states.reshape(2, 64, 512),
        log_sums.reshape(4, 4, 128),
        deltas.reshape(4, 4, 128),
        hidden_in[0],
    )
    dq, dk, dv, kw, vw = pl.pallas_call(
        finish_kernel,
        out_shape=(
            struct((128, 2048), BF),
            struct((128, 512), BF),
            struct((128, 512), BF),
            struct((8, 512), F32),
            struct((8, 512), F32),
        ),
        in_specs=[VMEM] * 3,
        out_specs=(VMEM,) * 5,
        name="finish",
    )(dqh, kvg, wout)
    return (dq[None], dk[None], dv[None], kw, vw)


def solution(mesh):
    tokens, rows = P("batch", "seq", None), P("batch", None, "seq")
    return jax.shard_map(
        shards,
        mesh=mesh,
        in_specs=(tokens, tokens, tokens, tokens, tokens, rows, rows, P()),
        out_specs=(tokens, tokens, tokens, P(("batch", "seq"), None), P(("batch", "seq"), None)),
        check_vma=False,
    )
```
